32 devices in a mesh: det: 8 (over y, x, core), bm: 4 (over z).
Axes of the slice: x: 2, y: 2, z: 4, core: 2. Of those that a mesh axis runs over, the one named last changes fastest.
Arguments:
- sky_alm: bfloat16 [2, 3, 16, 128], P(None, None, 'det'), may hold values from -6 to 6
- beam_blm: bfloat16 [2, 3, 16, 128], P(None, None, 'bm'), may hold values from -2.5 to 2.5
- wigner: bfloat16 [32, 16, 16, 128], P('det', None, 'bm'), may hold values from -0.03125 to 0.03125
- theta_index: int32 [128, 256], P('det'), may hold values from 0 to 3
- phi_index: int32 [128, 256], P('det'), may hold values from 0 to 16383
- psi_index: int32 [128, 256], P('det'), may hold values from 0 to 31
Outputs:
- tod: float32 [128, 256], P('det', 'bm')
The draws below stay inside these ranges and needn't reach their ends.
All inputs are finite; a program needn't handle non-finite values.
Results may differ from the reference program's by a relative error of at most 0.0029.
Values may be sent and summed in bfloat16 or wider, within the bound.
A program may use at most 64 MiB of HBM per device.

```python
import math
import jax
import jax.numpy as jnp
from jax import lax

LBAND = 128
BEAM_M = 16
NR = 4
SAMP = 256
NPHI = 16384
NPSI = 32
MWIN = 16
CYCLES = 32
DETS = 128
N_DET = 8


def set_ends(drawn, own_key, least, top_value):
    spot = [jax.random.randint(jax.random.fold_in(own_key, axis), (), 0, length) for axis, length in enumerate(drawn.shape)]
    main_axis = drawn.shape.index(max(drawn.shape))
    beside = spot[:main_axis] + [(spot[main_axis] + 1) % drawn.shape[main_axis]] + spot[main_axis + 1:]
    return drawn.at[tuple(spot)].set(least).at[tuple(beside)].set(top_value)


def shard_levels(stream_key, shape, cuts, least, high):
    level, own = 1.0, jax.random.fold_in(stream_key, 6)
    for axis_at, parts in cuts:
        draws = jnp.exp(jax.random.uniform(jax.random.fold_in(own, axis_at), (parts,), jnp.float32, least / len(cuts), high / len(cuts)))
        level = level * jnp.repeat(draws, shape[axis_at] // parts).reshape([-1 if axis == axis_at else 1 for axis in range(len(shape))])
    return level


def bell_draw(rng, extent, deviation, bound, split=(), kind=jnp.bfloat16):
    drawn = deviation * jax.random.normal(rng, extent, jnp.float32)
    if split:
        drawn = drawn * shard_levels(rng, extent, split, -0.22, 0.18)
    return jnp.clip(drawn, -bound, bound).astype(kind)


def setup_inputs(seed: int = 0) -> dict:
    splits = jax.random.split(jax.random.key(seed), 7)
    sky_alm = bell_draw(splits[0], (2, 3, MWIN, LBAND), 1.0, 6.0, ((2, 8),))
    beam_blm = bell_draw(splits[1], (2, 3, BEAM_M, LBAND), 6 ** -0.5, 2.5, ((2, 4),))
    wigner = bell_draw(splits[2], (CYCLES, MWIN, BEAM_M, LBAND), (LBAND * MWIN * BEAM_M) ** -0.5, 0.03125, ((0, 8), (2, 4)))
    theta_index = set_ends(jax.random.randint(splits[3], (DETS, SAMP), 0, NR), jax.random.fold_in(splits[3], 1), 0, NR - 1).astype(jnp.int32)
    phi_index = set_ends(jax.random.randint(splits[4], (DETS, SAMP), 0, NPHI), jax.random.fold_in(splits[4], 1), 0, NPHI - 1).astype(jnp.int32)
    psi_index = set_ends(jax.random.randint(splits[5], (DETS, SAMP), 0, NPSI), jax.random.fold_in(splits[5], 1), 0, NPSI - 1).astype(jnp.int32)
    return dict(sky_alm=sky_alm, beam_blm=beam_blm, wigner=wigner, theta_index=theta_index, phi_index=phi_index, psi_index=psi_index)


TWO_PI = 2.0 * math.pi


def spectra_of(sky, beam):
    sky_full = sky.astype(jnp.float32)[:, :, :, None, :]
    beam_full = beam.astype(jnp.float32)[:, :, None, :, :]
    real_part = jnp.sum(sky_full[0] * beam_full[0] - sky_full[1] * beam_full[1], axis=0)
    imag_part = jnp.sum(sky_full[0] * beam_full[1] + sky_full[1] * beam_full[0], axis=0)
    return jnp.stack([real_part, imag_part]).astype(jnp.bfloat16)


def product_first(left, right):
    dims = (((0,), (0,)), ((), ()))
    return lax.dot_general(left, right, dims, precision=lax.Precision.HIGHEST, preferred_element_type=jnp.float32)


def sample_tod(cube, theta, phi, psi, first_plane):
    cycles = cube.shape[1]
    planes = cube.shape[2]
    modes = cube.shape[3]
    plane_ids = first_plane + jnp.arange(planes, dtype=jnp.int32)
    psi_angle = TWO_PI * ((plane_ids[:, None] * psi[None, :]) % NPSI).astype(jnp.float32) / NPSI
    select = (theta[None, :] == jnp.arange(cycles, dtype=jnp.int32)[:, None]).astype(jnp.float32)
    cos_feat = (select[:, None, :] * jnp.cos(psi_angle)[None]).reshape(cycles * planes, -1)
    sin_feat = (select[:, None, :] * jnp.sin(psi_angle)[None]).reshape(cycles * planes, -1)
    flat = cube.reshape(2, cycles * planes, modes)
    k_real = product_first(flat[0], cos_feat) - product_first(flat[1], sin_feat)
    k_imag = product_first(flat[1], cos_feat) + product_first(flat[0], sin_feat)
    mode_ids = jnp.arange(modes, dtype=jnp.int32)
    phi_angle = TWO_PI * ((mode_ids[:, None] * phi[None, :]) % NPHI).astype(jnp.float32) / NPHI
    return jnp.sum(k_real * jnp.cos(phi_angle) - k_imag * jnp.sin(phi_angle), axis=0)


def reference(sky_alm, beam_blm, wigner, theta_index, phi_index, psi_index):
    spectra = lax.optimization_barrier(spectra_of(sky_alm, beam_blm)).astype(jnp.float32)
    tables = wigner.reshape(N_DET, NR, MWIN, BEAM_M, LBAND)

    def one_group(inputs):
        table, theta, phi, psi = inputs
        cube = jnp.einsum("rmpl,kmpl->krpm", table.astype(jnp.float32), spectra, precision=lax.Precision.HIGHEST)
        return sample_tod(cube, theta, phi, psi, 0)

    tod = lax.map(one_group, (tables, theta_index.reshape(N_DET, -1), phi_index.reshape(N_DET, -1), psi_index.reshape(N_DET, -1)))
    return tod.reshape(DETS, SAMP)
```

```python
import functools
import math

import jax
import jax.numpy as jnp
from jax import lax
from jax.experimental import pallas as pl
from jax.experimental.pallas import tpu as pltpu
from jax.sharding import PartitionSpec as P

NPHI = 16384
NPSI = 32

TWO_PI = 2.0 * math.pi
LANES = 128
ROWS = 8
PUSH_BYTES = 1 << 18
F32 = jnp.float32
BF16 = jnp.bfloat16
MESH = pl.DeviceIdType.MESH


def cos_on_grid(step, grid):
    shift = (grid // 4).bit_length() - 1
    turn = (step + grid // 8) >> shift
    x = (step - (turn << shift)).astype(F32) * (TWO_PI / grid)
    x2 = x * x
    c = 1.0 + x2 * (-0.5 + x2 * (1 / 24 + x2 * (-1 / 720 + x2 * (1 / 40320))))
    s = x * (1.0 + x2 * (-1 / 6 + x2 * (1 / 120 + x2 * (-1 / 5040 + x2 * (1 / 362880)))))
    odd = (turn & 1) == 1
    value = jnp.where(odd, -s, c)
    return jnp.where((turn & 2) == 2, -value, value)


def partner(me, flip, n):
    out, bit = 0, 1
    while bit < n:
        digit = (me // bit) % 2
        out = out + bit * ((1 - digit) if flip & bit else digit)
        bit *= 2
    return out


def rows_of(values, groups, width):
    return jnp.concatenate([values[j * ROWS : (j + 1) * ROWS] for j in range(groups)], axis=1)


def pushed(even, n_bm, source, target):
    return (even & (source > target) & (target == 0)) | (source - target >= n_bm - 1)


def kernel(
    n_det, n_bm, cycles, pushes,
    sky_hbm, beam_hbm, wig_hbm, theta_hbm, phi_hbm, psi_hbm, out_ref,
    sky_all, slab, index, sky_wide, wide, feat, phase, cube_all,
    local_sem, sky_sem, col_send, col_recv, ok, hello,
):
    det = lax.axis_index("det")
    bm = lax.axis_index("bm")
    even = det % 2 == 0
    pair = det // 2
    buddy = det + 1 - 2 * (det % 2)
    n_pairs = n_det // 2

    rows, band = slab.shape[1:]
    beam_rows = beam_hbm.shape[0]
    wig_rows = rows - beam_rows
    planes = beam_rows // 6
    flat = wig_rows // cycles
    modes = flat // planes
    owned = sky_all.shape[3]
    pairs = cycles * planes
    depth = 2 * pairs
    per_tile = LANES // (2 * depth)
    tile_modes = per_tile * ROWS
    tiles = modes // tile_modes
    dets, samples = index.shape[1:]
    width = samples // n_bm
    groups = dets // ROWS

    pltpu.make_async_copy(sky_hbm, sky_all.at[det], local_sem.at[0]).start()
    for g in range(cycles):
        part = pl.ds(g * flat, flat)
        pltpu.make_async_copy(wig_hbm.at[part], slab.at[bm, part], local_sem.at[1]).start()
    pltpu.make_async_copy(beam_hbm, slab.at[bm, pl.ds(wig_rows, beam_rows)], local_sem.at[1]).start()
    pltpu.make_async_copy(theta_hbm, index.at[0], local_sem.at[2]).start()
    pltpu.make_async_copy(phi_hbm, index.at[1], local_sem.at[2]).start()
    pltpu.make_async_copy(psi_hbm, index.at[2], local_sem.at[2]).start()

    barrier = pltpu.get_barrier_semaphore()

    def greet(semaphore, to_det, to_bm):
        pl.semaphore_signal(semaphore, inc=1, device_id=(to_det, to_bm), device_id_type=MESH)

    greet(barrier, buddy, bm)
    for z in range(1, n_bm):
        @pl.when(bm < z)
        def _():
            greet(barrier, 2 * pair + 1, z)
    for k in range(1, n_pairs):
        greet(barrier, 2 * ((pair + k) % n_pairs), bm)

    def push_to(z):
        return pltpu.make_async_remote_copy(
            src_ref=slab.at[bm], dst_ref=slab.at[bm],
            send_sem=col_send.at[z], recv_sem=col_recv.at[bm],
            device_id=(det, z), device_id_type=MESH,
        )

    def cube_to(z):
        return pltpu.make_async_remote_copy(
            src_ref=cube_all.at[bm], dst_ref=cube_all.at[bm],
            send_sem=col_send.at[z], recv_sem=col_recv.at[bm],
            device_id=(det, z), device_id_type=MESH,
        )

    def landing(buffer, z):
        return pltpu.make_async_remote_copy(
            src_ref=buffer.at[z], dst_ref=buffer.at[z],
            send_sem=col_send.at[z], recv_sem=col_recv.at[z],
            device_id=(det, z), device_id_type=MESH,
        )

    @pl.when(jnp.logical_not(even))
    def _():
        pl.semaphore_wait(barrier, 1 + 2 * bm)
        greet(ok, buddy, bm)

    def share_sky():
        @pl.when(even)
        def _():
            pl.semaphore_wait(barrier, n_det - 1)
            greet(ok, buddy, bm)

        @pl.when(jnp.logical_not(even))
        def _():
            pl.semaphore_wait(ok, 1)

        pltpu.make_async_copy(sky_hbm, sky_all.at[det], local_sem.at[0]).wait()
        for flip in range(n_det - 1, 0, -1):
            pltpu.make_async_remote_copy(
                src_ref=sky_all.at[det], dst_ref=sky_all.at[det],
                send_sem=sky_sem.at[0], recv_sem=sky_sem.at[1],
                device_id=(partner(det, flip, n_det), bm), device_id_type=MESH,
            ).start()

    def share_slab():
        @pl.when(even)
        def _():
            pl.semaphore_wait(ok, 1)

        for z in range(n_bm - 1):
            @pl.when(bm > z)
            def _():
                greet(hello, det, z)
        pltpu.make_async_copy(slab.at[bm], slab.at[bm], local_sem.at[1]).wait()
        if pushes:
            for z in range(n_bm - 1):
                @pl.when(pushed(even, n_bm, bm, z))
                def _():
                    push_to(z).start()

    last = pair == n_pairs - 1

    @pl.when(last)
    def _():
        share_sky()

    share_slab()

    @pl.when(jnp.logical_not(last))
    def _():
        share_sky()

    others = sky_all.at[pl.ds(0, n_det - 1)]
    skies = pltpu.make_async_remote_copy(
        src_ref=others, dst_ref=others,
        send_sem=sky_sem.at[0], recv_sem=sky_sem.at[1],
        device_id=(buddy, bm), device_id_type=MESH,
    )
    pltpu.make_async_copy(index, index, local_sem.at[2]).wait()

    def widen(z):
        for g in range(cycles):
            wide[g] = slab[z, pl.ds(g * flat, flat)].astype(F32)

    def mine(values):
        own = values[:, :width]
        for i in range(1, n_bm):
            own = jnp.where(bm == i, values[:, i * width : (i + 1) * width], own)
        return rows_of(own, groups, width)

    theta, phi, psi = mine(index[0]), mine(index[1]), mine(index[2])
    span = groups * width
    k_rows = n_bm * depth
    row = lax.broadcasted_iota(jnp.int32, (k_rows, span), 0)
    plane = row // depth * planes + row % planes
    cycle = (row // planes) % cycles
    quarter = ((row // pairs) % 2) * (3 * NPSI // 4)
    m_rows = 2 * modes
    mrow = lax.broadcasted_iota(jnp.int32, (m_rows, span), 0)
    mode = (mrow // (2 * tile_modes)) * tile_modes + mrow % tile_modes
    mquarter = ((mrow // tile_modes) % 2) * (NPHI // 4)
    for j in range(ROWS):
        at = pl.ds(j * span, span)
        step = (plane * psi[j : j + 1] + quarter) & (NPSI - 1)
        value = jnp.where(cycle == theta[j : j + 1], cos_on_grid(step, NPSI), 0.0)
        high = value.astype(BF16)
        feat[:k_rows, at] = high
        feat[k_rows:, at] = (value - high.astype(F32)).astype(BF16)
        step = (mode * phi[j : j + 1] + mquarter) & (NPHI - 1)
        phase[:, at] = cos_on_grid(step, NPHI)

    widen(bm)
    skies.wait_recv()

    slots = tile_modes // owned
    for t in range(tiles):
        for r in range(2):
            for c in range(3):
                sky_wide[r, c, pl.ds(t * tile_modes, tile_modes)] = (
                    sky_all[t * slots : (t + 1) * slots, r, c].astype(F32).reshape(tile_modes, band)
                )

    lane = lax.broadcasted_iota(jnp.int32, (ROWS, LANES), 1)
    imag_row = (lane // (depth * per_tile)) % 2
    sin_column = (lane // pairs) % 2
    part = (imag_row + sin_column) % 2
    code = ((lane // depth) % per_tile * 2 + part) * pairs + lane % pairs
    sign = jnp.where((imag_row == 0) & (sin_column == 1), -1.0, 1.0)

    def profile(z):
        beam = slab[z, pl.ds(wig_rows, beam_rows)].astype(F32)
        for t in range(tiles):
            packed = jnp.zeros((ROWS, LANES), F32)
            for h in range(per_tile):
                at = t * tile_modes + h * ROWS
                sky = [[sky_wide[r, c, pl.ds(at, ROWS)] for c in range(3)] for r in range(2)]
                for p in range(planes):
                    re = im = 0.0
                    for c in range(3):
                        b0 = beam[c * planes + p : c * planes + p + 1]
                        b1 = beam[(3 + c) * planes + p : (3 + c) * planes + p + 1]
                        re = re + (sky[0][c] * b0 - sky[1][c] * b1)
                        im = im + (sky[0][c] * b1 + sky[1][c] * b0)
                    re = re.astype(BF16).astype(F32)
                    im = im.astype(BF16).astype(F32)
                    for g in range(cycles):
                        w = wide[g, pl.ds(at * planes + p, ROWS, stride=planes)]
                        for k, spectra in enumerate((re, im)):
                            total = jnp.sum(w * spectra, axis=1, keepdims=True)
                            where = (h * 2 + k) * pairs + g * planes + p
                            packed = jnp.where(code == where, total, packed)
            cube_all[z, t] = packed * sign

    profile(bm)

    @pl.when(bm < n_bm - 1)
    def _():
        pl.semaphore_wait(hello, n_bm - 1 - bm)

    def by_cube(source, target):
        apart = source != target
        return apart & jnp.logical_not(pushed(even, n_bm, source, target)) if pushes else apart

    for z in range(n_bm - 1, -1, -1):
        @pl.when(by_cube(bm, z))
        def _():
            cube_to(z).start()

    for z in range(n_bm):
        @pl.when(by_cube(z, bm))
        def _():
            landing(cube_all, z).wait_recv()
        if pushes and z > 0:
            @pl.when(pushed(even, n_bm, z, bm))
            def _():
                landing(slab, z).wait_recv()
                widen(z)
                profile(z)

    blocks = []
    for t in range(tiles):
        parts = [cube_all[s, t] for s in range(n_bm)]
        for q in range(2 * per_tile):
            blocks.append(
                jnp.concatenate([x[:, q * depth : (q + 1) * depth] for x in parts], axis=1)
            )
    left = jnp.concatenate(blocks, axis=0)
    high = left.astype(BF16)
    low = (left - high.astype(F32)).astype(BF16)
    both = jnp.concatenate(
        [jnp.concatenate([high, high], axis=1), jnp.concatenate([low, low], axis=1)], axis=0
    )
    y = jnp.dot(both, feat[...], preferred_element_type=F32)
    z = (y[:m_rows] + y[m_rows:]) * phase[...]
    total = jnp.sum(z, axis=0, keepdims=True)
    for j in range(ROWS):
        for i in range(groups):
            at = j * span + i * width
            out_ref[pl.ds(i * ROWS + j, 1), :] = total[:, at : at + width]

    skies.wait_send()
    for z in range(n_bm):
        @pl.when(by_cube(bm, z))
        def _():
            cube_to(z).wait_send()
        if pushes and z < n_bm - 1:
            @pl.when(pushed(even, n_bm, bm, z))
            def _():
                push_to(z).wait_send()


def on_device(sky_alm, beam_blm, wigner, theta_index, phi_index, psi_index):
    n_det, n_bm = lax.axis_size("det"), lax.axis_size("bm")
    cycles, modes, planes, band = wigner.shape
    dets, samples = theta_index.shape
    width = samples // n_bm
    span = dets // ROWS * width
    depth = 2 * cycles * planes
    tiles = modes * 2 * depth // (ROWS * LANES)
    beam_rows = 6 * planes
    wig_rows = cycles * modes * planes
    pushes = 2 * wig_rows * band <= PUSH_BYTES
    any_space = pl.BlockSpec(memory_space=pl.ANY)
    return pl.pallas_call(
        functools.partial(kernel, n_det, n_bm, cycles, pushes),
        out_shape=pltpu.VMEM((dets, width), F32),
        in_specs=[any_space] * 6,
        out_specs=pl.BlockSpec(memory_space=pltpu.VMEM),
        scratch_shapes=[
            pltpu.VMEM((n_det, *sky_alm.shape), BF16),
            pltpu.VMEM((n_bm, wig_rows + beam_rows, band), BF16),
            pltpu.VMEM((3, dets, samples), jnp.int32),
            pltpu.VMEM((2, 3, modes, band), F32),
            pltpu.VMEM((cycles, modes * planes, band), F32),
            pltpu.VMEM((2 * n_bm * depth, ROWS * span), BF16),
            pltpu.VMEM((2 * modes, ROWS * span), F32),
            pltpu.VMEM((n_bm, tiles, ROWS, LANES), F32),
            pltpu.SemaphoreType.DMA((3,)),
            pltpu.SemaphoreType.DMA((2,)),
            pltpu.SemaphoreType.DMA((n_bm,)),
            pltpu.SemaphoreType.DMA((n_bm,)),
            pltpu.SemaphoreType.REGULAR,
            pltpu.SemaphoreType.REGULAR,
        ],
        compiler_params=pltpu.CompilerParams(collective_id=0, has_side_effects=True),
    )(
        sky_alm,
        beam_blm.reshape(beam_rows, band),
        wigner.reshape(wig_rows, band),
        theta_index,
        phi_index,
        psi_index,
    )


def solution(mesh):
    placed = (
        P(None, None, "det", None),
        P(None, None, "bm", None),
        P("det", None, "bm", None),
        P("det", None),
        P("det", None),
        P("det", None),
    )
    return jax.shard_map(
        on_device, mesh=mesh, in_specs=placed, out_specs=P("det", "bm"), check_vma=False
    )
```

```python
import functools
import math

import jax
import jax.numpy as jnp
from jax import lax
from jax.experimental import pallas as pl
from jax.experimental.pallas import tpu as pltpu
from jax.sharding import PartitionSpec as P

NPHI = 16384
NPSI = 32

TWO_PI = 2.0 * math.pi
LANES = 128
ROWS = 8
PUSH_BYTES = 1 << 18
F32 = jnp.float32
BF16 = jnp.bfloat16
MESH = pl.DeviceIdType.MESH


def cos_on_grid(step, grid):
    shift = (grid // 4).bit_length() - 1
    turn = (step + grid // 8) >> shift
    x = (step - (turn << shift)).astype(F32) * (TWO_PI / grid)
    x2 = x * x
    c = 1.0 + x2 * (-0.5 + x2 * (1 / 24 + x2 * (-1 / 720 + x2 * (1 / 40320))))
    s = x * (1.0 + x2 * (-1 / 6 + x2 * (1 / 120 + x2 * (-1 / 5040 + x2 * (1 / 362880)))))
    odd = (turn & 1) == 1
    value = jnp.where(odd, -s, c)
    return jnp.where((turn & 2) == 2, -value, value)


def partner(me, flip, n):
    out, bit = 0, 1
    while bit < n:
        digit = (me // bit) % 2
        out = out + bit * ((1 - digit) if flip & bit else digit)
        bit *= 2
    return out


def rows_of(values, groups, width):
    return jnp.concatenate([values[j * ROWS : (j + 1) * ROWS] for j in range(groups)], axis=1)


def pushed(even, n_bm, source, target):
    return (even & (source > target) & (target == 0)) | (source - target >= n_bm - 1)


def kernel(
    n_det, n_bm, cycles, pushes,
    sky_hbm, beam_hbm, wig_hbm, theta_hbm, phi_hbm, psi_hbm, out_ref,
    sky_all, slab, index, sky_wide, wide, feat, phase, cube_all, left,
    local_sem, sky_sem, col_send, col_recv, ok, hello,
):
    det = lax.axis_index("det")
    bm = lax.axis_index("bm")
    even = det % 2 == 0
    pair = det // 2
    buddy = det + 1 - 2 * (det % 2)
    n_pairs = n_det // 2

    rows, band = slab.shape[1:]
    beam_rows = beam_hbm.shape[0]
    wig_rows = rows - beam_rows
    planes = beam_rows // 6
    flat = wig_rows // cycles
    modes = flat // planes
    owned = sky_all.shape[3]
    pairs = cycles * planes
    depth = 2 * pairs
    per_tile = LANES // (2 * depth)
    tile_modes = per_tile * ROWS
    tiles = modes // tile_modes
    dets, samples = index.shape[1:]
    width = samples // n_bm
    groups = dets // ROWS

    pltpu.make_async_copy(sky_hbm, sky_all.at[det], local_sem.at[0]).start()
    for g in range(cycles):
        part = pl.ds(g * flat, flat)
        pltpu.make_async_copy(wig_hbm.at[part], slab.at[bm, part], local_sem.at[1]).start()
    pltpu.make_async_copy(beam_hbm, slab.at[bm, pl.ds(wig_rows, beam_rows)], local_sem.at[1]).start()
    pltpu.make_async_copy(theta_hbm, index.at[0], local_sem.at[2]).start()
    pltpu.make_async_copy(phi_hbm, index.at[1], local_sem.at[2]).start()
    pltpu.make_async_copy(psi_hbm, index.at[2], local_sem.at[2]).start()

    barrier = pltpu.get_barrier_semaphore()

    def greet(semaphore, to_det, to_bm):
        pl.semaphore_signal(semaphore, inc=1, device_id=(to_det, to_bm), device_id_type=MESH)

    greet(barrier, buddy, bm)
    for z in range(1, n_bm):
        @pl.when(bm < z)
        def _():
            greet(barrier, 2 * pair + 1, z)
    for k in range(1, n_pairs):
        greet(barrier, 2 * ((pair + k) % n_pairs), bm)

    def push_to(z):
        return pltpu.make_async_remote_copy(
            src_ref=slab.at[bm], dst_ref=slab.at[bm],
            send_sem=col_send.at[z], recv_sem=col_recv.at[bm],
            device_id=(det, z), device_id_type=MESH,
        )

    def cube_to(z):
        return pltpu.make_async_remote_copy(
            src_ref=cube_all.at[bm], dst_ref=cube_all.at[bm],
            send_sem=col_send.at[z], recv_sem=col_recv.at[bm],
            device_id=(det, z), device_id_type=MESH,
        )

    def landing(buffer, z):
        return pltpu.make_async_remote_copy(
            src_ref=buffer.at[z], dst_ref=buffer.at[z],
            send_sem=col_send.at[z], recv_sem=col_recv.at[z],
            device_id=(det, z), device_id_type=MESH,
        )

    @pl.when(jnp.logical_not(even))
    def _():
        pl.semaphore_wait(barrier, 1 + 2 * bm)
        greet(ok, buddy, bm)

    def share_sky():
        @pl.when(even)
        def _():
            pl.semaphore_wait(barrier, n_det - 1)
            greet(ok, buddy, bm)

        @pl.when(jnp.logical_not(even))
        def _():
            pl.semaphore_wait(ok, 1)

        pltpu.make_async_copy(sky_hbm, sky_all.at[det], local_sem.at[0]).wait()
        for flip in range(n_det - 1, 0, -1):
            pltpu.make_async_remote_copy(
                src_ref=sky_all.at[det], dst_ref=sky_all.at[det],
                send_sem=sky_sem.at[0], recv_sem=sky_sem.at[1],
                device_id=(partner(det, flip, n_det), bm), device_id_type=MESH,
            ).start()

    def share_slab():
        @pl.when(even)
        def _():
            pl.semaphore_wait(ok, 1)

        for z in range(n_bm - 1):
            @pl.when(bm > z)
            def _():
                greet(hello, det, z)
        pltpu.make_async_copy(slab.at[bm], slab.at[bm], local_sem.at[1]).wait()
        if pushes:
            for z in range(n_bm - 1):
                @pl.when(pushed(even, n_bm, bm, z))
                def _():
                    push_to(z).start()

    last = pair == n_pairs - 1

    @pl.when(last)
    def _():
        share_sky()

    share_slab()

    @pl.when(jnp.logical_not(last))
    def _():
        share_sky()

    others = sky_all.at[pl.ds(0, n_det - 1)]
    skies = pltpu.make_async_remote_copy(
        src_ref=others, dst_ref=others,
        send_sem=sky_sem.at[0], recv_sem=sky_sem.at[1],
        device_id=(buddy, bm), device_id_type=MESH,
    )
    pltpu.make_async_copy(index, index, local_sem.at[2]).wait()

    def widen(z):
        for g in range(cycles):
            wide[g] = slab[z, pl.ds(g * flat, flat)].astype(F32)

    def mine(values):
        own = values[:, :width]
        for i in range(1, n_bm):
            own = jnp.where(bm == i, values[:, i * width : (i + 1) * width], own)
        return rows_of(own, groups, width)

    theta, phi, psi = mine(index[0]), mine(index[1]), mine(index[2])
    span = groups * width
    k_rows = n_bm * depth
    row = lax.broadcasted_iota(jnp.int32, (k_rows, span), 0)
    plane = row // depth * planes + row % planes
    cycle = (row // planes) % cycles
    quarter = ((row // pairs) % 2) * (3 * NPSI // 4)
    m_rows = 2 * modes
    mrow = lax.broadcasted_iota(jnp.int32, (m_rows, span), 0)
    mode = (mrow // (2 * tile_modes)) * tile_modes + mrow % tile_modes
    mquarter = ((mrow // tile_modes) % 2) * (NPHI // 4)
    for j in range(ROWS):
        at = pl.ds(j * span, span)
        step = (plane * psi[j : j + 1] + quarter) & (NPSI - 1)
        value = jnp.where(cycle == theta[j : j + 1], cos_on_grid(step, NPSI), 0.0)
        feat[:, at] = value.astype(BF16)
        step = (mode * phi[j : j + 1] + mquarter) & (NPHI - 1)
        phase[:, at] = cos_on_grid(step, NPHI)

    widen(bm)
    skies.wait_recv()

    slots = tile_modes // owned
    for t in range(tiles):
        for r in range(2):
            for c in range(3):
                sky_wide[r, c, pl.ds(t * tile_modes, tile_modes)] = (
                    sky_all[t * slots : (t + 1) * slots, r, c].astype(F32).reshape(tile_modes, band)
                )

    lane = lax.broadcasted_iota(jnp.int32, (ROWS, LANES), 1)
    blocks = 2 * per_tile
    imag_row = (lane // (depth * per_tile)) % 2
    sin_column = (lane // pairs) % 2
    part = (imag_row + sin_column) % 2
    code = ((lane // depth) % per_tile * 2 + part) * pairs + lane % pairs
    sign = jnp.where((imag_row == 0) & (sin_column == 1), -1.0, 1.0)
    sign_column = jnp.where(sin_column == 1, -1.0, 1.0)

    def totals(z, t, h):
        beam = slab[z, pl.ds(wig_rows, beam_rows)].astype(F32)
        at = t * tile_modes + h * ROWS
        sky = [[sky_wide[r, c, pl.ds(at, ROWS)] for c in range(3)] for r in range(2)]
        for p in range(planes):
            re = im = 0.0
            for c in range(3):
                b0 = beam[c * planes + p : c * planes + p + 1]
                b1 = beam[(3 + c) * planes + p : (3 + c) * planes + p + 1]
                re = re + (sky[0][c] * b0 - sky[1][c] * b1)
                im = im + (sky[0][c] * b1 + sky[1][c] * b0)
            re = re.astype(BF16).astype(F32)
            im = im.astype(BF16).astype(F32)
            for g in range(cycles):
                w = wide[g, pl.ds(at * planes + p, ROWS, stride=planes)]
                for k, spectra in enumerate((re, im)):
                    yield k, g * planes + p, jnp.sum(w * spectra, axis=1, keepdims=True)

    def profile(z):
        for t in range(tiles):
            packed = jnp.zeros((ROWS, LANES), F32)
            for h in range(per_tile):
                for k, i, total in totals(z, t, h):
                    packed = jnp.where(code == (h * 2 + k) * pairs + i, total, packed)
            cube_all[z, t] = packed * sign

    def profile_here(z):
        inner = lane - z * depth
        inside = lane // depth == z
        for t in range(tiles):
            for h in range(per_tile):
                real = imag = jnp.zeros((ROWS, LANES), F32)
                for k, i, total in totals(z, t, h):
                    cos_place, sin_place = inner == i, inner == pairs + i
                    real = jnp.where(sin_place if k else cos_place, total, real)
                    imag = jnp.where(cos_place if k else sin_place, total, imag)
                left[t, h] = jnp.where(inside, real * sign_column, left[t, h])
                left[t, per_tile + h] = jnp.where(inside, imag, left[t, per_tile + h])

    def place(z):
        inside = lane // depth == z
        for t in range(tiles):
            for q in range(blocks):
                moved = pltpu.roll(cube_all[z, t], (z - q) % n_bm * depth, 1)
                left[t, q] = jnp.where(inside, moved, left[t, q])

    profile(bm)

    @pl.when(bm < n_bm - 1)
    def _():
        pl.semaphore_wait(hello, n_bm - 1 - bm)

    def by_cube(source, target):
        apart = source != target
        return apart & jnp.logical_not(pushed(even, n_bm, source, target)) if pushes else apart

    for z in range(n_bm - 1, -1, -1):
        @pl.when(by_cube(bm, z))
        def _():
            cube_to(z).start()

    left[...] = jnp.zeros_like(left)
    for z in range(n_bm):
        @pl.when(bm == z)
        def _():
            place(z)

    if pushes:
        for z in range(1, n_bm):
            @pl.when(pushed(even, n_bm, z, bm))
            def _():
                landing(slab, z).wait_recv()
                widen(z)
                profile_here(z)

    for z in range(n_bm):
        @pl.when(by_cube(z, bm))
        def _():
            landing(cube_all, z).wait_recv()
            place(z)

    wave = left[...].reshape(m_rows, k_rows)
    high = wave.astype(BF16)
    low = (wave - high.astype(F32)).astype(BF16)
    both = jnp.concatenate([high, low], axis=0)
    y = jnp.dot(both, feat[...], preferred_element_type=F32)
    z = (y[:m_rows] + y[m_rows:]) * phase[...]
    total = jnp.sum(z, axis=0, keepdims=True)
    for j in range(ROWS):
        for i in range(groups):
            at = j * span + i * width
            out_ref[pl.ds(i * ROWS + j, 1), :] = total[:, at : at + width]

    skies.wait_send()
    for z in range(n_bm):
        @pl.when(by_cube(bm, z))
        def _():
            cube_to(z).wait_send()
        if pushes and z < n_bm - 1:
            @pl.when(pushed(even, n_bm, bm, z))
            def _():
                push_to(z).wait_send()


def on_device(sky_alm, beam_blm, wigner, theta_index, phi_index, psi_index):
    n_det, n_bm = lax.axis_size("det"), lax.axis_size("bm")
    cycles, modes, planes, band = wigner.shape
    dets, samples = theta_index.shape
    width = samples // n_bm
    span = dets // ROWS * width
    depth = 2 * cycles * planes
    tiles = modes * 2 * depth // (ROWS * LANES)
    beam_rows = 6 * planes
    wig_rows = cycles * modes * planes
    pushes = 2 * wig_rows * band <= PUSH_BYTES
    any_space = pl.BlockSpec(memory_space=pl.ANY)
    return pl.pallas_call(
        functools.partial(kernel, n_det, n_bm, cycles, pushes),
        out_shape=pltpu.VMEM((dets, width), F32),
        in_specs=[any_space] * 6,
        out_specs=pl.BlockSpec(memory_space=pltpu.VMEM),
        scratch_shapes=[
            pltpu.VMEM((n_det, *sky_alm.shape), BF16),
            pltpu.VMEM((n_bm, wig_rows + beam_rows, band), BF16),
            pltpu.VMEM((3, dets, samples), jnp.int32),
            pltpu.VMEM((2, 3, modes, band), F32),
            pltpu.VMEM((cycles, modes * planes, band), F32),
            pltpu.VMEM((n_bm * depth, ROWS * span), BF16),
            pltpu.VMEM((2 * modes, ROWS * span), F32),
            pltpu.VMEM((n_bm, tiles, ROWS, LANES), F32),
            pltpu.VMEM((tiles, LANES // depth, ROWS, LANES), F32),
            pltpu.SemaphoreType.DMA((3,)),
            pltpu.SemaphoreType.DMA((2,)),
            pltpu.SemaphoreType.DMA((n_bm,)),
            pltpu.SemaphoreType.DMA((n_bm,)),
            pltpu.SemaphoreType.REGULAR,
            pltpu.SemaphoreType.REGULAR,
        ],
        compiler_params=pltpu.CompilerParams(collective_id=0, has_side_effects=True),
    )(
        sky_alm,
        beam_blm.reshape(beam_rows, band),
        wigner.reshape(wig_rows, band),
        theta_index,
        phi_index,
        psi_index,
    )


def solution(mesh):
    placed = (
        P(None, None, "det", None),
        P(None, None, "bm", None),
        P("det", None, "bm", None),
        P("det", None),
        P("det", None),
        P("det", None),
    )
    return jax.shard_map(
        on_device, mesh=mesh, in_specs=placed, out_specs=P("det", "bm"), check_vma=False
    )
```

```python
import functools
import math

import jax
import jax.numpy as jnp
from jax import lax
from jax.experimental import pallas as pl
from jax.experimental.pallas import tpu as pltpu
from jax.sharding import PartitionSpec as P

NPHI = 16384
NPSI = 32

TWO_PI = 2.0 * math.pi
LANES = 128
ROWS = 8
PUSH_BYTES = 1 << 18
F32 = jnp.float32
BF16 = jnp.bfloat16
MESH = pl.DeviceIdType.MESH


def cos_on_grid(step, grid):
    shift = (grid // 4).bit_length() - 1
    turn = (step + grid // 8) >> shift
    x = (step - (turn << shift)).astype(F32) * (TWO_PI / grid)
    x2 = x * x
    c = 1.0 + x2 * (-0.5 + x2 * (1 / 24 + x2 * (-1 / 720 + x2 * (1 / 40320))))
    s = x * (1.0 + x2 * (-1 / 6 + x2 * (1 / 120 + x2 * (-1 / 5040 + x2 * (1 / 362880)))))
    odd = (turn & 1) == 1
    value = jnp.where(odd, -s, c)
    return jnp.where((turn & 2) == 2, -value, value)


def partner(me, flip, n):
    out, bit = 0, 1
    while bit < n:
        digit = (me // bit) % 2
        out = out + bit * ((1 - digit) if flip & bit else digit)
        bit *= 2
    return out


def rows_of(values, groups, width):
    return jnp.concatenate([values[j * ROWS : (j + 1) * ROWS] for j in range(groups)], axis=1)


def pushed(even, source, target):
    return (source - target >= 2) | (even & (source > target) & (target == 0))


def kernel(
    n_det, n_bm, modes, pushes,
    sky_hbm, beam_hbm, wig_hbm, theta_hbm, phi_hbm, psi_hbm, out_ref,
    sky_all, slab, index, sky_wide, wide, feat, phase, cube_all, early, left,
    local_sem, sky_sem, col_send, col_recv, ok, hello,
):
    det = lax.axis_index("det")
    bm = lax.axis_index("bm")
    even = det % 2 == 0
    pair = det // 2
    buddy = det + 1 - 2 * (det % 2)
    n_pairs = n_det // 2

    cycles, units, _, band = wig_hbm.shape
    beam_units = beam_hbm.shape[0]
    planes = beam_units * ROWS // 6
    owned = sky_all.shape[3]
    chunks = n_pairs if pushes else 1
    part_units = units // chunks
    chunk_units = cycles * part_units
    wig_units = cycles * units
    pairs = cycles * planes
    depth = 2 * pairs
    per_tile = LANES // (2 * depth)
    tile_modes = per_tile * ROWS
    tiles = modes // tile_modes
    dets, samples = index.shape[1:]
    width = samples // n_bm
    groups = dets // ROWS

    pltpu.make_async_copy(sky_hbm, sky_all.at[det], local_sem.at[0]).start()

    def place_of(k):
        return partner(pair, k, n_pairs) if pushes else 0

    def fetch(k):
        pltpu.make_async_copy(
            wig_hbm.at[:, pl.ds(place_of(k) * part_units, part_units)],
            slab.at[bm, pl.ds(k * chunk_units, chunk_units)].reshape(cycles, part_units, ROWS, band),
            local_sem.at[2 + k],
        ).start()

    for k in range(1, chunks):
        fetch(k)
    pltpu.make_async_copy(
        beam_hbm, slab.at[bm, pl.ds(wig_units, beam_units)], local_sem.at[1 + chunks]
    ).start()
    fetch(0)

    barrier = pltpu.get_barrier_semaphore()

    def greet(semaphore, to_det, to_bm):
        pl.semaphore_signal(semaphore, inc=1, device_id=(to_det, to_bm), device_id_type=MESH)

    greet(barrier, buddy, bm)
    for z in range(1, n_bm):
        @pl.when(bm < z)
        def _():
            greet(barrier, 2 * pair + 1, z)
    for k in range(1, n_pairs):
        greet(barrier, 2 * ((pair + k) % n_pairs), bm)
    pltpu.make_async_copy(theta_hbm, index.at[0], local_sem.at[1]).start()
    pltpu.make_async_copy(phi_hbm, index.at[1], local_sem.at[1]).start()
    pltpu.make_async_copy(psi_hbm, index.at[2], local_sem.at[1]).start()

    def units_of(first, stop):
        end = wig_units + beam_units if stop == chunks else stop * chunk_units
        return pl.ds(first * chunk_units, end - first * chunk_units)

    def push_to(z, first=1, stop=chunks):
        part = slab.at[bm, units_of(first, stop)]
        return pltpu.make_async_remote_copy(
            src_ref=part, dst_ref=part,
            send_sem=col_send.at[z], recv_sem=col_recv.at[bm],
            device_id=(det, z), device_id_type=MESH,
        )

    def early_to(z):
        return pltpu.make_async_remote_copy(
            src_ref=early.at[bm], dst_ref=early.at[bm],
            send_sem=col_send.at[z], recv_sem=col_recv.at[bm],
            device_id=(det, z), device_id_type=MESH,
        )

    def cube_to(z):
        return pltpu.make_async_remote_copy(
            src_ref=cube_all.at[bm], dst_ref=cube_all.at[bm],
            send_sem=col_send.at[z], recv_sem=col_recv.at[bm],
            device_id=(det, z), device_id_type=MESH,
        )

    def landing(buffer, z):
        return pltpu.make_async_remote_copy(
            src_ref=buffer, dst_ref=buffer,
            send_sem=col_send.at[z], recv_sem=col_recv.at[z],
            device_id=(det, z), device_id_type=MESH,
        )

    early_units = ROWS * LANES * 4 // (ROWS * band * 2)
    moved = slab.at[bm, pl.ds(0, wig_units + beam_units - chunk_units + early_units)]

    @pl.when(jnp.logical_not(even))
    def _():
        pl.semaphore_wait(barrier, 1 + 2 * bm)
        greet(ok, buddy, bm)

    @pl.when(even)
    def _():
        pl.semaphore_wait(ok, 1)

    pltpu.make_async_copy(sky_hbm, sky_all.at[det], local_sem.at[0]).wait()
    to_buddy = pltpu.make_async_remote_copy(
        src_ref=sky_all.at[det], dst_ref=sky_all.at[det],
        send_sem=sky_sem.at[2], recv_sem=sky_sem.at[3],
        device_id=(buddy, bm), device_id_type=MESH,
    )
    to_buddy.start()

    def share_sky():
        @pl.when(even)
        def _():
            pl.semaphore_wait(barrier, n_det - 1)
            greet(ok, buddy, bm)

        @pl.when(jnp.logical_not(even))
        def _():
            pl.semaphore_wait(ok, 1)

        for flip in range(n_det - 1, 1, -1):
            pltpu.make_async_remote_copy(
                src_ref=sky_all.at[det], dst_ref=sky_all.at[det],
                send_sem=sky_sem.at[0], recv_sem=sky_sem.at[1],
                device_id=(partner(det, flip, n_det), bm), device_id_type=MESH,
            ).start()

    lane = lax.broadcasted_iota(jnp.int32, (ROWS, LANES), 1)
    blocks = 2 * per_tile
    imag_row = (lane // (depth * per_tile)) % 2
    sin_column = (lane // pairs) % 2
    part = (imag_row + sin_column) % 2
    code = ((lane // depth) % per_tile * 2 + part) * pairs + lane % pairs
    sign = jnp.where((imag_row == 0) & (sin_column == 1), -1.0, 1.0)
    sign_column = jnp.where(sin_column == 1, -1.0, 1.0)

    def widen(z, first):
        for k in range(first, chunks):
            rows = pl.ds(pl.multiple_of(place_of(k) * part_units * ROWS, ROWS), part_units * ROWS)
            for g in range(cycles):
                block = slab[z, pl.ds(k * chunk_units + g * part_units, part_units)]
                wide[g, rows] = block.astype(F32).reshape(part_units * ROWS, band)

    def totals(z, sky, at):
        beam = slab[z, pl.ds(wig_units, beam_units)].astype(F32).reshape(beam_units * ROWS, band)
        for p in range(planes):
            re = im = 0.0
            for c in range(3):
                b0 = beam[c * planes + p : c * planes + p + 1]
                b1 = beam[(3 + c) * planes + p : (3 + c) * planes + p + 1]
                re = re + (sky[0][c] * b0 - sky[1][c] * b1)
                im = im + (sky[0][c] * b1 + sky[1][c] * b0)
            re = re.astype(BF16).astype(F32)
            im = im.astype(BF16).astype(F32)
            for g in range(cycles):
                w = wide[g, pl.ds(at * planes + p, ROWS, stride=planes)]
                for k, spectra in enumerate((re, im)):
                    yield k, g * planes + p, jnp.sum(w * spectra, axis=1, keepdims=True)

    shared = 2 * owned
    own_group = pair * shared // ROWS

    def send_early():
        to_buddy.wait_recv()
        near = [
            [
                sky_all[pl.ds(2 * pair, 2), r, c].astype(F32).reshape(shared, band)
                for c in range(3)
            ]
            for r in range(2)
        ]
        sky = [[jnp.concatenate([x] * (ROWS // shared), axis=0) for x in y] for y in near]
        packed = jnp.zeros((ROWS, LANES), F32)
        for k, i, total in totals(bm, sky, pl.multiple_of(own_group * ROWS, ROWS)):
            packed = jnp.where(part * pairs + lane % pairs == k * pairs + i, total, packed)
        early[bm] = packed * sign
        early_to(0).start()

    def share_slab():
        for k in [*range(1, chunks), 0]:
            part = slab.at[bm, units_of(k, k + 1)]
            pltpu.make_async_copy(part, part, local_sem.at[2 + k]).wait()
            if pushes and k:
                @pl.when(pushed(even, bm, 0))
                def _():
                    push_to(0, k, k + 1).start()
        for z in range(n_bm - 1):
            @pl.when(bm > z)
            def _():
                greet(hello, det, z)
        widen(bm, 0)
        if pushes:
            @pl.when(pushed(even, bm, 0))
            def _():
                send_early()

    last = pair == n_pairs - 1

    @pl.when(last)
    def _():
        share_sky()

    share_slab()

    @pl.when(jnp.logical_not(last))
    def _():
        share_sky()

    def share_inner(now):
        for z in range(1, n_bm - 1):
            @pl.when(now & pushed(even, bm, z))
            def _():
                push_to(z).start()
                early_to(z).start()

    if pushes:
        share_inner(pair == 0)

    others = sky_all.at[pl.ds(0, n_det - 2)]
    skies = pltpu.make_async_remote_copy(
        src_ref=others, dst_ref=others,
        send_sem=sky_sem.at[0], recv_sem=sky_sem.at[1],
        device_id=(buddy, bm), device_id_type=MESH,
    )
    pltpu.make_async_copy(index, index, local_sem.at[1]).wait()

    def mine(values):
        own = values[:, :width]
        for i in range(1, n_bm):
            own = jnp.where(bm == i, values[:, i * width : (i + 1) * width], own)
        return rows_of(own, groups, width)

    theta, phi, psi = mine(index[0]), mine(index[1]), mine(index[2])
    span = groups * width
    k_rows = n_bm * depth
    row = lax.broadcasted_iota(jnp.int32, (k_rows, span), 0)
    plane = row // depth * planes + row % planes
    cycle = (row // planes) % cycles
    quarter = ((row // pairs) % 2) * (3 * NPSI // 4)
    m_rows = 2 * modes
    mrow = lax.broadcasted_iota(jnp.int32, (m_rows, span), 0)
    mode = (mrow // (2 * tile_modes)) * tile_modes + mrow % tile_modes
    mquarter = ((mrow // tile_modes) % 2) * (NPHI // 4)
    for j in range(ROWS):
        at = pl.ds(j * span, span)
        step = (plane * psi[j : j + 1] + quarter) & (NPSI - 1)
        value = jnp.where(cycle == theta[j : j + 1], cos_on_grid(step, NPSI), 0.0)
        feat[:, at] = value.astype(BF16)
        step = (mode * phi[j : j + 1] + mquarter) & (NPHI - 1)
        phase[:, at] = cos_on_grid(step, NPHI)

    if pushes:
        share_inner(pair != 0)

        @pl.when(jnp.logical_not(pushed(even, bm, 0)))
        def _():
            to_buddy.wait_recv()
    else:
        to_buddy.wait_recv()
    skies.wait_recv()

    slots = tile_modes // owned
    for t in range(tiles):
        for r in range(2):
            for c in range(3):
                sky_wide[r, c, pl.ds(t * tile_modes, tile_modes)] = (
                    sky_all[t * slots : (t + 1) * slots, r, c].astype(F32).reshape(tile_modes, band)
                )

    def tile_totals(z, t, h):
        at = t * tile_modes + h * ROWS
        sky = [[sky_wide[r, c, pl.ds(at, ROWS)] for c in range(3)] for r in range(2)]
        return totals(z, sky, at)

    def profile(z):
        for t in range(tiles):
            packed = jnp.zeros((ROWS, LANES), F32)
            for h in range(per_tile):
                for k, i, total in tile_totals(z, t, h):
                    packed = jnp.where(code == (h * 2 + k) * pairs + i, total, packed)
            cube_all[z, t] = packed * sign

    def profile_here(z):
        inner = lane - z * depth
        inside = lane // depth == z
        for t in range(tiles):
            for h in range(per_tile):
                real = imag = jnp.zeros((ROWS, LANES), F32)
                for k, i, total in tile_totals(z, t, h):
                    cos_place, sin_place = inner == i, inner == pairs + i
                    real = jnp.where(sin_place if k else cos_place, total, real)
                    imag = jnp.where(cos_place if k else sin_place, total, imag)
                left[t, h] = jnp.where(inside, real * sign_column, left[t, h])
                left[t, per_tile + h] = jnp.where(inside, imag, left[t, per_tile + h])
        row = lax.broadcasted_iota(jnp.int32, (ROWS, LANES), 0)
        known = inside & (row // shared == pair % (ROWS // shared))
        for q in range(blocks):
            ready = pltpu.roll(early[z], (z - q) % n_bm * depth, 1)
            left[0, q] = jnp.where(known & (own_group == q % per_tile), ready, left[0, q])

    def place(z):
        inside = lane // depth == z
        for t in range(tiles):
            for q in range(blocks):
                moved = pltpu.roll(cube_all[z, t], (z - q) % n_bm * depth, 1)
                left[t, q] = jnp.where(inside, moved, left[t, q])

    profile(bm)

    @pl.when(bm < n_bm - 1)
    def _():
        pl.semaphore_wait(hello, n_bm - 1 - bm)

    def by_cube(source, target):
        apart = source != target
        return apart & jnp.logical_not(pushed(even, source, target)) if pushes else apart

    for z in range(n_bm - 1, -1, -1):
        @pl.when(by_cube(bm, z))
        def _():
            cube_to(z).start()

    left[...] = jnp.zeros_like(left)
    for z in range(n_bm):
        @pl.when(bm == z)
        def _():
            place(z)

    if pushes:
        for z in range(n_bm - 1, 0, -1):
            @pl.when(pushed(even, z, bm))
            def _():
                landing(moved, z).wait_recv()
                widen(z, 1)
                profile_here(z)

    for z in range(n_bm):
        @pl.when(by_cube(z, bm))
        def _():
            landing(cube_all.at[z], z).wait_recv()
            place(z)

    wave = left[...].reshape(m_rows, k_rows)
    high = wave.astype(BF16)
    low = (wave - high.astype(F32)).astype(BF16)
    both = jnp.concatenate([high, low], axis=0)
    y = jnp.dot(both, feat[...], preferred_element_type=F32)
    z = (y[:m_rows] + y[m_rows:]) * phase[...]
    total = jnp.sum(z, axis=0, keepdims=True)
    for j in range(ROWS):
        for i in range(groups):
            at = j * span + i * width
            out_ref[pl.ds(i * ROWS + j, 1), :] = total[:, at : at + width]

    skies.wait_send()
    to_buddy.wait_send()
    for z in range(n_bm):
        @pl.when(by_cube(bm, z))
        def _():
            cube_to(z).wait_send()
        if pushes and z < n_bm - 1:
            @pl.when(pushed(even, bm, z))
            def _():
                landing(moved, z).wait_send()


def on_device(sky_alm, beam_blm, wigner, theta_index, phi_index, psi_index):
    n_det, n_bm = lax.axis_size("det"), lax.axis_size("bm")
    cycles, modes, planes, band = wigner.shape
    dets, samples = theta_index.shape
    width = samples // n_bm
    span = dets // ROWS * width
    depth = 2 * cycles * planes
    tiles = modes * 2 * depth // (ROWS * LANES)
    beam_rows = 6 * planes
    units = modes * planes // ROWS
    wig_units = cycles * units
    beam_units = beam_rows // ROWS
    pushes = tiles == 1 and 2 * wig_units * ROWS * band <= PUSH_BYTES
    any_space = pl.BlockSpec(memory_space=pl.ANY)
    return pl.pallas_call(
        functools.partial(kernel, n_det, n_bm, modes, pushes),
        out_shape=pltpu.VMEM((dets, width), F32),
        in_specs=[any_space] * 6,
        out_specs=pl.BlockSpec(memory_space=pltpu.VMEM),
        scratch_shapes=[
            pltpu.VMEM((n_det, *sky_alm.shape), BF16),
            pltpu.VMEM((n_bm, wig_units + beam_units, ROWS, band), BF16),
            pltpu.VMEM((3, dets, samples), jnp.int32),
            pltpu.VMEM((2, 3, modes, band), F32),
            pltpu.VMEM((cycles, modes * planes, band), F32),
            pltpu.VMEM((n_bm * depth, ROWS * span), BF16),
            pltpu.VMEM((2 * modes, ROWS * span), F32),
            pltpu.VMEM((n_bm, tiles, ROWS, LANES), F32),
            pltpu.VMEM((n_bm, ROWS, LANES), F32),
            pltpu.VMEM((tiles, LANES // depth, ROWS, LANES), F32),
            pltpu.SemaphoreType.DMA((2 + (n_det // 2 if pushes else 1),)),
            pltpu.SemaphoreType.DMA((4,)),
            pltpu.SemaphoreType.DMA((n_bm,)),
            pltpu.SemaphoreType.DMA((n_bm,)),
            pltpu.SemaphoreType.REGULAR,
            pltpu.SemaphoreType.REGULAR,
        ],
        compiler_params=pltpu.CompilerParams(collective_id=0, has_side_effects=True),
    )(
        sky_alm,
        beam_blm.reshape(beam_units, ROWS, band),
        wigner.reshape(cycles, units, ROWS, band),
        theta_index,
        phi_index,
        psi_index,
    )


def solution(mesh):
    placed = (
        P(None, None, "det", None),
        P(None, None, "bm", None),
        P("det", None, "bm", None),
        P("det", None),
        P("det", None),
        P("det", None),
    )
    return jax.shard_map(
        on_device, mesh=mesh, in_specs=placed, out_specs=P("det", "bm"), check_vma=False
    )
```

```python
import functools
import math

import jax
import jax.numpy as jnp
from jax import lax
from jax.experimental import pallas as pl
from jax.experimental.pallas import tpu as pltpu
from jax.sharding import PartitionSpec as P

NPHI = 16384
NPSI = 32

TWO_PI = 2.0 * math.pi
LANES = 128
ROWS = 8
PUSH_BYTES = 1 << 18
F32 = jnp.float32
BF16 = jnp.bfloat16
MESH = pl.DeviceIdType.MESH


def cos_on_grid(step, grid):
    shift = (grid // 4).bit_length() - 1
    turn = (step + grid // 8) >> shift
    x = (step - (turn << shift)).astype(F32) * (TWO_PI / grid)
    x2 = x * x
    c = 1.0 + x2 * (-0.5 + x2 * (1 / 24 + x2 * (-1 / 720 + x2 * (1 / 40320))))
    s = x * (1.0 + x2 * (-1 / 6 + x2 * (1 / 120 + x2 * (-1 / 5040 + x2 * (1 / 362880)))))
    odd = (turn & 1) == 1
    value = jnp.where(odd, -s, c)
    return jnp.where((turn & 2) == 2, -value, value)


def partner(me, flip, n):
    out, bit = 0, 1
    while bit < n:
        digit = (me // bit) % 2
        out = out + bit * ((1 - digit) if flip & bit else digit)
        bit *= 2
    return out


def rows_of(values, groups, width):
    return jnp.concatenate([values[j * ROWS : (j + 1) * ROWS] for j in range(groups)], axis=1)


def pushed(role, source, target):
    even, inner = role
    near = even & (source > target) & (target == 0)
    return near | ((source - target >= 2) & (inner | (target == 0)))


def kernel(
    n_det, n_bm, modes, pushes,
    sky_hbm, beam_hbm, wig_hbm, theta_hbm, phi_hbm, psi_hbm, out_ref,
    sky_all, slab, index, sky_wide, wide, feat, phase, cube_all, early, left,
    local_sem, sky_sem, col_send, col_recv, ok, hello,
):
    det = lax.axis_index("det")
    bm = lax.axis_index("bm")
    even = det % 2 == 0
    pair = det // 2
    buddy = det + 1 - 2 * (det % 2)
    n_pairs = n_det // 2
    role = even, even | (pair != n_pairs - 1)

    cycles, units, _, band = wig_hbm.shape
    beam_units = beam_hbm.shape[0]
    planes = beam_units * ROWS // 6
    owned = sky_all.shape[3]
    chunks = n_pairs if pushes else 1
    part_units = units // chunks
    chunk_units = cycles * part_units
    wig_units = cycles * units
    pairs = cycles * planes
    depth = 2 * pairs
    per_tile = LANES // (2 * depth)
    tile_modes = per_tile * ROWS
    tiles = modes // tile_modes
    dets, samples = index.shape[1:]
    width = samples // n_bm
    groups = dets // ROWS

    pltpu.make_async_copy(sky_hbm, sky_all.at[det], local_sem.at[0]).start()

    def place_of(k):
        return partner(pair, k, n_pairs) if pushes else 0

    def fetch(k):
        pltpu.make_async_copy(
            wig_hbm.at[:, pl.ds(place_of(k) * part_units, part_units)],
            slab.at[bm, pl.ds(k * chunk_units, chunk_units)].reshape(cycles, part_units, ROWS, band),
            local_sem.at[2 + k],
        ).start()

    for k in range(1, chunks):
        fetch(k)
    pltpu.make_async_copy(
        beam_hbm, slab.at[bm, pl.ds(wig_units, beam_units)], local_sem.at[1 + chunks]
    ).start()
    fetch(0)

    barrier = pltpu.get_barrier_semaphore()

    def greet(semaphore, to_det, to_bm):
        pl.semaphore_signal(semaphore, inc=1, device_id=(to_det, to_bm), device_id_type=MESH)

    greet(barrier, buddy, bm)
    for z in range(1, n_bm):
        @pl.when(bm < z)
        def _():
            greet(barrier, 2 * pair + 1, z)
    for k in range(1, n_pairs):
        greet(barrier, 2 * ((pair + k) % n_pairs), bm)
    pltpu.make_async_copy(theta_hbm, index.at[0], local_sem.at[1]).start()
    pltpu.make_async_copy(phi_hbm, index.at[1], local_sem.at[1]).start()
    pltpu.make_async_copy(psi_hbm, index.at[2], local_sem.at[1]).start()

    def units_of(first, stop):
        end = wig_units + beam_units if stop == chunks else stop * chunk_units
        return pl.ds(first * chunk_units, end - first * chunk_units)

    def push_to(z, first=1, stop=chunks):
        part = slab.at[bm, units_of(first, stop)]
        return pltpu.make_async_remote_copy(
            src_ref=part, dst_ref=part,
            send_sem=col_send.at[z], recv_sem=col_recv.at[bm],
            device_id=(det, z), device_id_type=MESH,
        )

    def early_to(z):
        return pltpu.make_async_remote_copy(
            src_ref=early.at[bm], dst_ref=early.at[bm],
            send_sem=col_send.at[z], recv_sem=col_recv.at[bm],
            device_id=(det, z), device_id_type=MESH,
        )

    def cube_to(z):
        return pltpu.make_async_remote_copy(
            src_ref=cube_all.at[bm], dst_ref=cube_all.at[bm],
            send_sem=col_send.at[z], recv_sem=col_recv.at[bm],
            device_id=(det, z), device_id_type=MESH,
        )

    def landing(buffer, z):
        return pltpu.make_async_remote_copy(
            src_ref=buffer, dst_ref=buffer,
            send_sem=col_send.at[z], recv_sem=col_recv.at[z],
            device_id=(det, z), device_id_type=MESH,
        )

    early_units = ROWS * LANES * 4 // (ROWS * band * 2)
    moved = slab.at[bm, pl.ds(0, wig_units + beam_units - chunk_units + early_units)]

    @pl.when(jnp.logical_not(even))
    def _():
        pl.semaphore_wait(barrier, 1 + 2 * bm)
        greet(ok, buddy, bm)

    @pl.when(even)
    def _():
        pl.semaphore_wait(ok, 1)

    pltpu.make_async_copy(sky_hbm, sky_all.at[det], local_sem.at[0]).wait()
    to_buddy = pltpu.make_async_remote_copy(
        src_ref=sky_all.at[det], dst_ref=sky_all.at[det],
        send_sem=sky_sem.at[2], recv_sem=sky_sem.at[3],
        device_id=(buddy, bm), device_id_type=MESH,
    )
    to_buddy.start()

    def share_sky():
        @pl.when(even)
        def _():
            pl.semaphore_wait(barrier, n_det - 1)
            greet(ok, buddy, bm)

        @pl.when(jnp.logical_not(even))
        def _():
            pl.semaphore_wait(ok, 1)

        for flip in range(n_det - 1, 1, -1):
            pltpu.make_async_remote_copy(
                src_ref=sky_all.at[det], dst_ref=sky_all.at[det],
                send_sem=sky_sem.at[0], recv_sem=sky_sem.at[1],
                device_id=(partner(det, flip, n_det), bm), device_id_type=MESH,
            ).start()

    lane = lax.broadcasted_iota(jnp.int32, (ROWS, LANES), 1)
    blocks = 2 * per_tile
    imag_row = (lane // (depth * per_tile)) % 2
    sin_column = (lane // pairs) % 2
    part = (imag_row + sin_column) % 2
    code = ((lane // depth) % per_tile * 2 + part) * pairs + lane % pairs
    sign = jnp.where((imag_row == 0) & (sin_column == 1), -1.0, 1.0)
    sign_column = jnp.where(sin_column == 1, -1.0, 1.0)

    def widen(z, first):
        for k in range(first, chunks):
            rows = pl.ds(pl.multiple_of(place_of(k) * part_units * ROWS, ROWS), part_units * ROWS)
            for g in range(cycles):
                block = slab[z, pl.ds(k * chunk_units + g * part_units, part_units)]
                wide[g, rows] = block.astype(F32).reshape(part_units * ROWS, band)

    def totals(z, sky, at):
        beam = slab[z, pl.ds(wig_units, beam_units)].astype(F32).reshape(beam_units * ROWS, band)
        for p in range(planes):
            re = im = 0.0
            for c in range(3):
                b0 = beam[c * planes + p : c * planes + p + 1]
                b1 = beam[(3 + c) * planes + p : (3 + c) * planes + p + 1]
                re = re + (sky[0][c] * b0 - sky[1][c] * b1)
                im = im + (sky[0][c] * b1 + sky[1][c] * b0)
            re = re.astype(BF16).astype(F32)
            im = im.astype(BF16).astype(F32)
            for g in range(cycles):
                w = wide[g, pl.ds(at * planes + p, ROWS, stride=planes)]
                for k, spectra in enumerate((re, im)):
                    yield k, g * planes + p, jnp.sum(w * spectra, axis=1, keepdims=True)

    shared = 2 * owned
    own_group = pair * shared // ROWS

    def send_early():
        to_buddy.wait_recv()
        near = [
            [
                sky_all[pl.ds(2 * pair, 2), r, c].astype(F32).reshape(shared, band)
                for c in range(3)
            ]
            for r in range(2)
        ]
        sky = [[jnp.concatenate([x] * (ROWS // shared), axis=0) for x in y] for y in near]
        packed = jnp.zeros((ROWS, LANES), F32)
        for k, i, total in totals(bm, sky, pl.multiple_of(own_group * ROWS, ROWS)):
            packed = jnp.where(part * pairs + lane % pairs == k * pairs + i, total, packed)
        early[bm] = packed * sign
        early_to(0).start()

    yields = jnp.logical_not(even) & (pair == 0) & (bm == n_bm - 1)

    def share_slab():
        for k in [*range(1, chunks), 0]:
            part = slab.at[bm, units_of(k, k + 1)]
            pltpu.make_async_copy(part, part, local_sem.at[2 + k]).wait()
            if pushes and k:
                @pl.when(jnp.logical_not(yields) & pushed(role, bm, 0))
                def _():
                    push_to(0, k, k + 1).start()
        for z in range(n_bm - 1):
            @pl.when(bm > z)
            def _():
                greet(hello, det, z)
        widen(bm, 0)
        if pushes:
            @pl.when(pushed(role, bm, 0))
            def _():
                send_early()

            @pl.when(yields & pushed(role, bm, 0))
            def _():
                push_to(0).start()

    last = pair == n_pairs - 1

    @pl.when(last)
    def _():
        share_sky()

    share_slab()

    @pl.when(jnp.logical_not(last))
    def _():
        share_sky()

    def share_inner(now):
        for z in range(1, n_bm - 1):
            @pl.when(now & pushed(role, bm, z))
            def _():
                push_to(z).start()
                early_to(z).start()

    if pushes:
        share_inner((pair == 0) | jnp.logical_not(even))

    others = sky_all.at[pl.ds(0, n_det - 2)]
    skies = pltpu.make_async_remote_copy(
        src_ref=others, dst_ref=others,
        send_sem=sky_sem.at[0], recv_sem=sky_sem.at[1],
        device_id=(buddy, bm), device_id_type=MESH,
    )
    pltpu.make_async_copy(index, index, local_sem.at[1]).wait()

    def mine(values):
        own = values[:, :width]
        for i in range(1, n_bm):
            own = jnp.where(bm == i, values[:, i * width : (i + 1) * width], own)
        return rows_of(own, groups, width)

    theta, phi, psi = mine(index[0]), mine(index[1]), mine(index[2])
    span = groups * width
    k_rows = n_bm * depth
    row = lax.broadcasted_iota(jnp.int32, (k_rows, span), 0)
    plane = row // depth * planes + row % planes
    cycle = (row // planes) % cycles
    quarter = ((row // pairs) % 2) * (3 * NPSI // 4)
    m_rows = 2 * modes
    mrow = lax.broadcasted_iota(jnp.int32, (m_rows, span), 0)
    mode = (mrow // (2 * tile_modes)) * tile_modes + mrow % tile_modes
    mquarter = ((mrow // tile_modes) % 2) * (NPHI // 4)
    for j in range(ROWS):
        at = pl.ds(j * span, span)
        step = (plane * psi[j : j + 1] + quarter) & (NPSI - 1)
        value = jnp.where(cycle == theta[j : j + 1], cos_on_grid(step, NPSI), 0.0)
        feat[:, at] = value.astype(BF16)
        step = (mode * phi[j : j + 1] + mquarter) & (NPHI - 1)
        phase[:, at] = cos_on_grid(step, NPHI)

    if pushes:
        share_inner((pair != 0) & even)

        @pl.when(jnp.logical_not(pushed(role, bm, 0)))
        def _():
            to_buddy.wait_recv()
    else:
        to_buddy.wait_recv()
    skies.wait_recv()

    slots = tile_modes // owned
    for t in range(tiles):
        for r in range(2):
            for c in range(3):
                sky_wide[r, c, pl.ds(t * tile_modes, tile_modes)] = (
                    sky_all[t * slots : (t + 1) * slots, r, c].astype(F32).reshape(tile_modes, band)
                )

    def tile_totals(z, t, h):
        at = t * tile_modes + h * ROWS
        sky = [[sky_wide[r, c, pl.ds(at, ROWS)] for c in range(3)] for r in range(2)]
        return totals(z, sky, at)

    def profile(z):
        for t in range(tiles):
            packed = jnp.zeros((ROWS, LANES), F32)
            for h in range(per_tile):
                for k, i, total in tile_totals(z, t, h):
                    packed = jnp.where(code == (h * 2 + k) * pairs + i, total, packed)
            cube_all[z, t] = packed * sign

    def profile_here(z):
        inner = lane - z * depth
        inside = lane // depth == z
        for t in range(tiles):
            for h in range(per_tile):
                real = imag = jnp.zeros((ROWS, LANES), F32)
                for k, i, total in tile_totals(z, t, h):
                    cos_place, sin_place = inner == i, inner == pairs + i
                    real = jnp.where(sin_place if k else cos_place, total, real)
                    imag = jnp.where(cos_place if k else sin_place, total, imag)
                left[t, h] = jnp.where(inside, real * sign_column, left[t, h])
                left[t, per_tile + h] = jnp.where(inside, imag, left[t, per_tile + h])
        row = lax.broadcasted_iota(jnp.int32, (ROWS, LANES), 0)
        known = inside & (row // shared == pair % (ROWS // shared))
        for q in range(blocks):
            ready = pltpu.roll(early[z], (z - q) % n_bm * depth, 1)
            left[0, q] = jnp.where(known & (own_group == q % per_tile), ready, left[0, q])

    def place(z):
        inside = lane // depth == z
        for t in range(tiles):
            for q in range(blocks):
                moved = pltpu.roll(cube_all[z, t], (z - q) % n_bm * depth, 1)
                left[t, q] = jnp.where(inside, moved, left[t, q])

    profile(bm)

    @pl.when(bm < n_bm - 1)
    def _():
        pl.semaphore_wait(hello, n_bm - 1 - bm)

    def by_cube(source, target):
        apart = source != target
        return apart & jnp.logical_not(pushed(role, source, target)) if pushes else apart

    for z in range(n_bm - 1, -1, -1):
        @pl.when(by_cube(bm, z))
        def _():
            cube_to(z).start()

    left[...] = jnp.zeros_like(left)
    for z in range(n_bm):
        @pl.when(bm == z)
        def _():
            place(z)

    if pushes:
        for z in range(1, n_bm):
            @pl.when(pushed(role, z, bm))
            def _():
                landing(moved, z).wait_recv()
                widen(z, 1)
                profile_here(z)

    for z in range(n_bm):
        @pl.when(by_cube(z, bm))
        def _():
            landing(cube_all.at[z], z).wait_recv()
            place(z)

    wave = left[...].reshape(m_rows, k_rows)
    high = wave.astype(BF16)
    low = (wave - high.astype(F32)).astype(BF16)
    both = jnp.concatenate([high, low], axis=0)
    y = jnp.dot(both, feat[...], preferred_element_type=F32)
    z = (y[:m_rows] + y[m_rows:]) * phase[...]
    total = jnp.sum(z, axis=0, keepdims=True)
    for j in range(ROWS):
        for i in range(groups):
            at = j * span + i * width
            out_ref[pl.ds(i * ROWS + j, 1), :] = total[:, at : at + width]

    skies.wait_send()
    to_buddy.wait_send()
    for z in range(n_bm):
        @pl.when(by_cube(bm, z))
        def _():
            cube_to(z).wait_send()
        if pushes and z < n_bm - 1:
            @pl.when(pushed(role, bm, z))
            def _():
                landing(moved, z).wait_send()


def on_device(sky_alm, beam_blm, wigner, theta_index, phi_index, psi_index):
    n_det, n_bm = lax.axis_size("det"), lax.axis_size("bm")
    cycles, modes, planes, band = wigner.shape
    dets, samples = theta_index.shape
    width = samples // n_bm
    span = dets // ROWS * width
    depth = 2 * cycles * planes
    tiles = modes * 2 * depth // (ROWS * LANES)
    beam_rows = 6 * planes
    units = modes * planes // ROWS
    wig_units = cycles * units
    beam_units = beam_rows // ROWS
    pushes = tiles == 1 and 2 * wig_units * ROWS * band <= PUSH_BYTES
    any_space = pl.BlockSpec(memory_space=pl.ANY)
    return pl.pallas_call(
        functools.partial(kernel, n_det, n_bm, modes, pushes),
        out_shape=pltpu.VMEM((dets, width), F32),
        in_specs=[any_space] * 6,
        out_specs=pl.BlockSpec(memory_space=pltpu.VMEM),
        scratch_shapes=[
            pltpu.VMEM((n_det, *sky_alm.shape), BF16),
            pltpu.VMEM((n_bm, wig_units + beam_units, ROWS, band), BF16),
            pltpu.VMEM((3, dets, samples), jnp.int32),
            pltpu.VMEM((2, 3, modes, band), F32),
            pltpu.VMEM((cycles, modes * planes, band), F32),
            pltpu.VMEM((n_bm * depth, ROWS * span), BF16),
            pltpu.VMEM((2 * modes, ROWS * span), F32),
            pltpu.VMEM((n_bm, tiles, ROWS, LANES), F32),
            pltpu.VMEM((n_bm, ROWS, LANES), F32),
            pltpu.VMEM((tiles, LANES // depth, ROWS, LANES), F32),
            pltpu.SemaphoreType.DMA((2 + (n_det // 2 if pushes else 1),)),
            pltpu.SemaphoreType.DMA((4,)),
            pltpu.SemaphoreType.DMA((n_bm,)),
            pltpu.SemaphoreType.DMA((n_bm,)),
            pltpu.SemaphoreType.REGULAR,
            pltpu.SemaphoreType.REGULAR,
        ],
        compiler_params=pltpu.CompilerParams(collective_id=0, has_side_effects=True),
    )(
        sky_alm,
        beam_blm.reshape(beam_units, ROWS, band),
        wigner.reshape(cycles, units, ROWS, band),
        theta_index,
        phi_index,
        psi_index,
    )


def solution(mesh):
    placed = (
        P(None, None, "det", None),
        P(None, None, "bm", None),
        P("det", None, "bm", None),
        P("det", None),
        P("det", None),
        P("det", None),
    )
    return jax.shard_map(
        on_device, mesh=mesh, in_specs=placed, out_specs=P("det", "bm"), check_vma=False
    )
```

```python
import functools
import math

import jax
import jax.numpy as jnp
from jax import lax
from jax.experimental import pallas as pl
from jax.experimental.pallas import tpu as pltpu
from jax.sharding import PartitionSpec as P

NPHI = 16384
NPSI = 32

TWO_PI = 2.0 * math.pi
LANES = 128
ROWS = 8
PUSH_BYTES = 1 << 18
F32 = jnp.float32
BF16 = jnp.bfloat16
MESH = pl.DeviceIdType.MESH


def cos_on_grid(step, grid):
    shift = (grid // 4).bit_length() - 1
    turn = (step + grid // 8) >> shift
    x = (step - (turn << shift)).astype(F32) * (TWO_PI / grid)
    x2 = x * x
    c = 1.0 + x2 * (-0.5 + x2 * (1 / 24 + x2 * (-1 / 720 + x2 * (1 / 40320))))
    s = x * (1.0 + x2 * (-1 / 6 + x2 * (1 / 120 + x2 * (-1 / 5040 + x2 * (1 / 362880)))))
    odd = (turn & 1) == 1
    value = jnp.where(odd, -s, c)
    return jnp.where((turn & 2) == 2, -value, value)


def partner(me, flip, n):
    out, bit = 0, 1
    while bit < n:
        digit = (me // bit) % 2
        out = out + bit * ((1 - digit) if flip & bit else digit)
        bit *= 2
    return out


def rows_of(values, groups, width):
    return jnp.concatenate([values[j * ROWS : (j + 1) * ROWS] for j in range(groups)], axis=1)


def pushed(role, n_bm, source, target):
    even, inner = role
    top = even & (source == n_bm - 1)
    return (source > target) & ((target == 0) | top | (inner & (source - target >= 2)))


def kernel(
    n_det, n_bm, modes, pushes,
    sky_hbm, beam_hbm, wig_hbm, theta_hbm, phi_hbm, psi_hbm, out_ref,
    sky_all, slab, index, sky_wide, wide, feat, phase, cube_all, early, left,
    sky_sem, col_send, col_recv, ok, hello,
):
    det = lax.axis_index("det")
    bm = lax.axis_index("bm")
    even = det % 2 == 0
    pair = det // 2
    buddy = det + 1 - 2 * (det % 2)
    n_pairs = n_det // 2
    role = even, even | (pair != n_pairs - 1)

    cycles, units, _, band = wig_hbm.shape
    beam_units = beam_hbm.shape[0]
    planes = beam_units * ROWS // 6
    owned = sky_all.shape[3]
    chunks = n_pairs if pushes else 1
    part_units = units // chunks
    chunk_units = cycles * part_units
    wig_units = cycles * units
    pairs = cycles * planes
    depth = 2 * pairs
    per_tile = LANES // (2 * depth)
    tile_modes = per_tile * ROWS
    tiles = modes // tile_modes
    dets, samples = index.shape[1:]
    width = samples // n_bm
    groups = dets // ROWS

    load = pltpu.make_async_copy(sky_hbm, sky_all.at[det], col_recv.at[bm])
    load.start()

    def place_of(k):
        return partner(pair, k, n_pairs) if pushes else 0

    def fetch(k):
        pltpu.make_async_copy(
            wig_hbm.at[:, pl.ds(place_of(k) * part_units, part_units)],
            slab.at[bm, pl.ds(k * chunk_units, chunk_units)].reshape(cycles, part_units, ROWS, band),
            col_send.at[bm],
        ).start()

    for k in range(1, chunks):
        fetch(k)
    pltpu.make_async_copy(
        beam_hbm, slab.at[bm, pl.ds(wig_units, beam_units)], col_send.at[bm]
    ).start()
    fetch(0)

    barrier = pltpu.get_barrier_semaphore()

    def greet(semaphore, to_det, to_bm):
        pl.semaphore_signal(semaphore, inc=1, device_id=(to_det, to_bm), device_id_type=MESH)

    greet(barrier, buddy, bm)
    for z in range(1, n_bm):
        @pl.when(bm < z)
        def _():
            greet(barrier, 2 * pair + 1, z)
    for k in range(1, n_pairs):
        greet(barrier, 2 * ((pair + k) % n_pairs), bm)

    sent = pl.ds(chunk_units, wig_units + beam_units - chunk_units)

    def push_to(z):
        return pltpu.make_async_remote_copy(
            src_ref=slab.at[bm, sent], dst_ref=slab.at[bm, sent],
            send_sem=col_send.at[z], recv_sem=col_recv.at[bm],
            device_id=(det, z), device_id_type=MESH,
        )

    def early_to(z):
        return pltpu.make_async_remote_copy(
            src_ref=early.at[bm], dst_ref=early.at[bm],
            send_sem=col_send.at[z], recv_sem=col_recv.at[bm],
            device_id=(det, z), device_id_type=MESH,
        )

    def cube_to(z):
        return pltpu.make_async_remote_copy(
            src_ref=cube_all.at[bm], dst_ref=cube_all.at[bm],
            send_sem=col_send.at[z], recv_sem=col_recv.at[bm],
            device_id=(det, z), device_id_type=MESH,
        )

    def landing(buffer, z):
        return pltpu.make_async_remote_copy(
            src_ref=buffer, dst_ref=buffer,
            send_sem=col_send.at[z], recv_sem=col_recv.at[z],
            device_id=(det, z), device_id_type=MESH,
        )

    early_units = ROWS * LANES * 4 // (ROWS * band * 2)
    moved = slab.at[bm, pl.ds(0, wig_units + beam_units - chunk_units + early_units)]

    @pl.when(jnp.logical_not(even))
    def _():
        pl.semaphore_wait(barrier, 1 + 2 * bm)
        greet(ok, buddy, bm)

    @pl.when(even)
    def _():
        pl.semaphore_wait(ok, 1)

    load.wait()
    to_buddy = pltpu.make_async_remote_copy(
        src_ref=sky_all.at[det], dst_ref=sky_all.at[det],
        send_sem=sky_sem.at[0], recv_sem=sky_sem.at[2],
        device_id=(buddy, bm), device_id_type=MESH,
    )
    to_buddy.start()
    pltpu.make_async_copy(theta_hbm, index.at[0], col_recv.at[bm]).start()
    pltpu.make_async_copy(phi_hbm, index.at[1], col_recv.at[bm]).start()
    pltpu.make_async_copy(psi_hbm, index.at[2], col_recv.at[bm]).start()

    def share_sky():
        @pl.when(even)
        def _():
            pl.semaphore_wait(barrier, n_det - 1)
            greet(ok, buddy, bm)

        @pl.when(jnp.logical_not(even))
        def _():
            pl.semaphore_wait(ok, 1)

        for flip in range(n_det - 1, 1, -1):
            pltpu.make_async_remote_copy(
                src_ref=sky_all.at[det], dst_ref=sky_all.at[det],
                send_sem=sky_sem.at[0], recv_sem=sky_sem.at[1],
                device_id=(partner(det, flip, n_det), bm), device_id_type=MESH,
            ).start()

    lane = lax.broadcasted_iota(jnp.int32, (ROWS, LANES), 1)
    blocks = 2 * per_tile
    imag_row = (lane // (depth * per_tile)) % 2
    sin_column = (lane // pairs) % 2
    part = (imag_row + sin_column) % 2
    code = ((lane // depth) % per_tile * 2 + part) * pairs + lane % pairs
    sign = jnp.where((imag_row == 0) & (sin_column == 1), -1.0, 1.0)
    sign_column = jnp.where(sin_column == 1, -1.0, 1.0)

    def widen(z, first):
        for k in range(first, chunks):
            rows = pl.ds(pl.multiple_of(place_of(k) * part_units * ROWS, ROWS), part_units * ROWS)
            for g in range(cycles):
                block = slab[z, pl.ds(k * chunk_units + g * part_units, part_units)]
                wide[g, rows] = block.astype(F32).reshape(part_units * ROWS, band)

    def totals(z, sky, at):
        beam = slab[z, pl.ds(wig_units, beam_units)].astype(F32).reshape(beam_units * ROWS, band)
        for p in range(planes):
            re = im = 0.0
            for c in range(3):
                b0 = beam[c * planes + p : c * planes + p + 1]
                b1 = beam[(3 + c) * planes + p : (3 + c) * planes + p + 1]
                re = re + (sky[0][c] * b0 - sky[1][c] * b1)
                im = im + (sky[0][c] * b1 + sky[1][c] * b0)
            re = re.astype(BF16).astype(F32)
            im = im.astype(BF16).astype(F32)
            for g in range(cycles):
                w = wide[g, pl.ds(at * planes + p, ROWS, stride=planes)]
                for k, spectra in enumerate((re, im)):
                    yield k, g * planes + p, jnp.sum(w * spectra, axis=1, keepdims=True)

    shared = 2 * owned
    own_group = pair * shared // ROWS

    def send_early():
        to_buddy.wait_recv()
        near = [
            [
                sky_all[pl.ds(2 * pair, 2), r, c].astype(F32).reshape(shared, band)
                for c in range(3)
            ]
            for r in range(2)
        ]
        sky = [[jnp.concatenate([x] * (ROWS // shared), axis=0) for x in y] for y in near]
        packed = jnp.zeros((ROWS, LANES), F32)
        for k, i, total in totals(bm, sky, pl.multiple_of(own_group * ROWS, ROWS)):
            packed = jnp.where(part * pairs + lane % pairs == k * pairs + i, total, packed)
        early[bm] = packed * sign
        early_to(0).start()

    yields = jnp.logical_not(even) & (pair == 0) & (bm == n_bm - 1)

    def share_slab():
        pltpu.make_async_copy(slab.at[bm], slab.at[bm], col_send.at[bm]).wait()
        if pushes:
            @pl.when(jnp.logical_not(yields) & pushed(role, n_bm, bm, 0))
            def _():
                push_to(0).start()
        for z in range(n_bm - 1):
            @pl.when(bm > z)
            def _():
                greet(hello, det, z)
        widen(bm, 0)
        if pushes:
            @pl.when(pushed(role, n_bm, bm, 0))
            def _():
                send_early()

            @pl.when(yields & pushed(role, n_bm, bm, 0))
            def _():
                push_to(0).start()

    last = pair == n_pairs - 1

    @pl.when(last)
    def _():
        share_sky()

    share_slab()

    @pl.when(jnp.logical_not(last))
    def _():
        share_sky()

    def share_inner(now):
        for z in range(1, n_bm - 1):
            @pl.when(now & pushed(role, n_bm, bm, z))
            def _():
                push_to(z).start()
                early_to(z).start()

    if pushes:
        share_inner((pair == 0) | jnp.logical_not(even))

    others = sky_all.at[pl.ds(0, n_det - 2)]
    skies = pltpu.make_async_remote_copy(
        src_ref=others, dst_ref=others,
        send_sem=sky_sem.at[0], recv_sem=sky_sem.at[1],
        device_id=(buddy, bm), device_id_type=MESH,
    )
    pltpu.make_async_copy(index, index, col_recv.at[bm]).wait()

    def mine(values):
        own = values[:, :width]
        for i in range(1, n_bm):
            own = jnp.where(bm == i, values[:, i * width : (i + 1) * width], own)
        return rows_of(own, groups, width)

    theta, phi, psi = mine(index[0]), mine(index[1]), mine(index[2])
    span = groups * width
    k_rows = n_bm * depth
    row = lax.broadcasted_iota(jnp.int32, (k_rows, span), 0)
    plane = row // depth * planes + row % planes
    cycle = (row // planes) % cycles
    quarter = ((row // pairs) % 2) * (3 * NPSI // 4)
    m_rows = 2 * modes
    mrow = lax.broadcasted_iota(jnp.int32, (m_rows, span), 0)
    mode = (mrow // (2 * tile_modes)) * tile_modes + mrow % tile_modes
    mquarter = ((mrow // tile_modes) % 2) * (NPHI // 4)
    for j in range(ROWS):
        at = pl.ds(j * span, span)
        step = (plane * psi[j : j + 1] + quarter) & (NPSI - 1)
        value = jnp.where(cycle == theta[j : j + 1], cos_on_grid(step, NPSI), 0.0)
        feat[:, at] = value.astype(BF16)
        step = (mode * phi[j : j + 1] + mquarter) & (NPHI - 1)
        phase[:, at] = cos_on_grid(step, NPHI)

    if pushes:
        share_inner((pair != 0) & even)

        @pl.when(jnp.logical_not(pushed(role, n_bm, bm, 0)))
        def _():
            to_buddy.wait_recv()
    else:
        to_buddy.wait_recv()
    skies.wait_recv()

    slots = tile_modes // owned
    for t in range(tiles):
        for r in range(2):
            for c in range(3):
                sky_wide[r, c, pl.ds(t * tile_modes, tile_modes)] = (
                    sky_all[t * slots : (t + 1) * slots, r, c].astype(F32).reshape(tile_modes, band)
                )

    def tile_totals(z, t, h):
        at = t * tile_modes + h * ROWS
        sky = [[sky_wide[r, c, pl.ds(at, ROWS)] for c in range(3)] for r in range(2)]
        return totals(z, sky, at)

    def profile(z):
        for t in range(tiles):
            packed = jnp.zeros((ROWS, LANES), F32)
            for h in range(per_tile):
                for k, i, total in tile_totals(z, t, h):
                    packed = jnp.where(code == (h * 2 + k) * pairs + i, total, packed)
            cube_all[z, t] = packed * sign

    def profile_here(z):
        inner = lane - z * depth
        inside = lane // depth == z
        for t in range(tiles):
            for h in range(per_tile):
                real = imag = jnp.zeros((ROWS, LANES), F32)
                for k, i, total in tile_totals(z, t, h):
                    cos_place, sin_place = inner == i, inner == pairs + i
                    real = jnp.where(sin_place if k else cos_place, total, real)
                    imag = jnp.where(cos_place if k else sin_place, total, imag)
                left[t, h] = jnp.where(inside, real * sign_column, left[t, h])
                left[t, per_tile + h] = jnp.where(inside, imag, left[t, per_tile + h])
        row = lax.broadcasted_iota(jnp.int32, (ROWS, LANES), 0)
        known = inside & (row // shared == pair % (ROWS // shared))
        for q in range(blocks):
            ready = pltpu.roll(early[z], (z - q) % n_bm * depth, 1)
            left[0, q] = jnp.where(known & (own_group == q % per_tile), ready, left[0, q])

    def place(z):
        inside = lane // depth == z
        for t in range(tiles):
            for q in range(blocks):
                moved = pltpu.roll(cube_all[z, t], (z - q) % n_bm * depth, 1)
                left[t, q] = jnp.where(inside, moved, left[t, q])

    profile(bm)

    @pl.when(bm < n_bm - 1)
    def _():
        pl.semaphore_wait(hello, n_bm - 1 - bm)

    def by_cube(source, target):
        apart = source != target
        return apart & jnp.logical_not(pushed(role, n_bm, source, target)) if pushes else apart

    for z in range(n_bm - 1, -1, -1):
        @pl.when(by_cube(bm, z))
        def _():
            cube_to(z).start()

    left[...] = jnp.zeros_like(left)
    for z in range(n_bm):
        @pl.when(bm == z)
        def _():
            place(z)

    if pushes:
        for z in range(1, n_bm):
            @pl.when(pushed(role, n_bm, z, bm))
            def _():
                landing(moved, z).wait_recv()
                widen(z, 1)
                profile_here(z)

    for z in range(n_bm):
        @pl.when(by_cube(z, bm))
        def _():
            landing(cube_all.at[z], z).wait_recv()
            place(z)

    wave = left[...].reshape(m_rows, k_rows)
    high = wave.astype(BF16)
    low = (wave - high.astype(F32)).astype(BF16)
    both = jnp.concatenate([high, low], axis=0)
    y = jnp.dot(both, feat[...], preferred_element_type=F32)
    z = (y[:m_rows] + y[m_rows:]) * phase[...]
    total = jnp.sum(z, axis=0, keepdims=True)
    for j in range(ROWS):
        for i in range(groups):
            at = j * span + i * width
            out_ref[pl.ds(i * ROWS + j, 1), :] = total[:, at : at + width]

    every = sky_all.at[pl.ds(0, n_det - 1)]
    outbound = pltpu.make_async_remote_copy(
        src_ref=every, dst_ref=every,
        send_sem=sky_sem.at[0], recv_sem=sky_sem.at[1],
        device_id=(buddy, bm), device_id_type=MESH,
    )
    outbound.wait_send()
    for z in range(n_bm):
        @pl.when(by_cube(bm, z))
        def _():
            cube_to(z).wait_send()
        if pushes and z < n_bm - 1:
            @pl.when(pushed(role, n_bm, bm, z))
            def _():
                landing(moved, z).wait_send()


def on_device(sky_alm, beam_blm, wigner, theta_index, phi_index, psi_index):
    n_det, n_bm = lax.axis_size("det"), lax.axis_size("bm")
    cycles, modes, planes, band = wigner.shape
    dets, samples = theta_index.shape
    width = samples // n_bm
    span = dets // ROWS * width
    depth = 2 * cycles * planes
    tiles = modes * 2 * depth // (ROWS * LANES)
    beam_rows = 6 * planes
    units = modes * planes // ROWS
    wig_units = cycles * units
    beam_units = beam_rows // ROWS
    pushes = tiles == 1 and 2 * wig_units * ROWS * band <= PUSH_BYTES
    any_space = pl.BlockSpec(memory_space=pl.ANY)
    return pl.pallas_call(
        functools.partial(kernel, n_det, n_bm, modes, pushes),
        out_shape=pltpu.VMEM((dets, width), F32),
        in_specs=[any_space] * 6,
        out_specs=pl.BlockSpec(memory_space=pltpu.VMEM),
        scratch_shapes=[
            pltpu.VMEM((n_det, *sky_alm.shape), BF16),
            pltpu.VMEM((n_bm, wig_units + beam_units, ROWS, band), BF16),
            pltpu.VMEM((3, dets, samples), jnp.int32),
            pltpu.VMEM((2, 3, modes, band), F32),
            pltpu.VMEM((cycles, modes * planes, band), F32),
            pltpu.VMEM((n_bm * depth, ROWS * span), BF16),
            pltpu.VMEM((2 * modes, ROWS * span), F32),
            pltpu.VMEM((n_bm, tiles, ROWS, LANES), F32),
            pltpu.VMEM((n_bm, ROWS, LANES), F32),
            pltpu.VMEM((tiles, LANES // depth, ROWS, LANES), F32),
            pltpu.SemaphoreType.DMA((3,)),
            pltpu.SemaphoreType.DMA((n_bm,)),
            pltpu.SemaphoreType.DMA((n_bm,)),
            pltpu.SemaphoreType.REGULAR,
            pltpu.SemaphoreType.REGULAR,
        ],
        compiler_params=pltpu.CompilerParams(collective_id=0, has_side_effects=True),
    )(
        sky_alm,
        beam_blm.reshape(beam_units, ROWS, band),
        wigner.reshape(cycles, units, ROWS, band),
        theta_index,
        phi_index,
        psi_index,
    )


def solution(mesh):
    placed = (
        P(None, None, "det", None),
        P(None, None, "bm", None),
        P("det", None, "bm", None),
        P("det", None),
        P("det", None),
        P("det", None),
    )
    return jax.shard_map(
        on_device, mesh=mesh, in_specs=placed, out_specs=P("det", "bm"), check_vma=False
    )
```

```python
import functools
import math

import jax
import jax.numpy as jnp
from jax import lax
from jax.experimental import pallas as pl
from jax.experimental.pallas import tpu as pltpu
from jax.sharding import PartitionSpec as P

NPHI = 16384
NPSI = 32

TWO_PI = 2.0 * math.pi
LANES = 128
ROWS = 8
PUSH_BYTES = 1 << 18
F32 = jnp.float32
BF16 = jnp.bfloat16
MESH = pl.DeviceIdType.MESH


def cos_on_grid(step, grid):
    shift = (grid // 4).bit_length() - 1
    turn = (step + grid // 8) >> shift
    x = (step - (turn << shift)).astype(F32) * (TWO_PI / grid)
    x2 = x * x
    c = 1.0 + x2 * (-0.5 + x2 * (1 / 24 + x2 * (-1 / 720 + x2 * (1 / 40320))))
    s = x * (1.0 + x2 * (-1 / 6 + x2 * (1 / 120 + x2 * (-1 / 5040 + x2 * (1 / 362880)))))
    odd = (turn & 1) == 1
    value = jnp.where(odd, -s, c)
    return jnp.where((turn & 2) == 2, -value, value)


def partner(me, flip, n):
    out, bit = 0, 1
    while bit < n:
        digit = (me // bit) % 2
        out = out + bit * ((1 - digit) if flip & bit else digit)
        bit *= 2
    return out


def rows_of(values, groups, width):
    return jnp.concatenate([values[j * ROWS : (j + 1) * ROWS] for j in range(groups)], axis=1)


def pushed(role, n_bm, source, target):
    even, inner = role
    top = even & (source == n_bm - 1)
    return (source > target) & ((target == 0) | top | (inner & (source - target >= 2)))


def kernel(
    n_det, n_bm, modes, pushes,
    sky_hbm, beam_hbm, wig_hbm, theta_hbm, phi_hbm, psi_hbm, out_ref,
    sky_all, slab, index, sky_wide, wide, feat, phase, cube_all, early, left,
    sky_sem, col_send, col_recv, ok, hello,
):
    det = lax.axis_index("det")
    bm = lax.axis_index("bm")
    even = det % 2 == 0
    pair = det // 2
    buddy = det + 1 - 2 * (det % 2)
    n_pairs = n_det // 2
    role = even, even | (pair != n_pairs - 1)

    cycles, units, _, band = wig_hbm.shape
    beam_units = beam_hbm.shape[0]
    planes = beam_units * ROWS // 6
    owned = sky_all.shape[3]
    chunks = n_pairs if pushes else 1
    part_units = units // chunks
    chunk_units = cycles * part_units
    wig_units = cycles * units
    pairs = cycles * planes
    depth = 2 * pairs
    per_tile = LANES // (2 * depth)
    tile_modes = per_tile * ROWS
    tiles = modes // tile_modes
    dets, samples = index.shape[1:]
    width = samples // n_bm
    groups = dets // ROWS

    load = pltpu.make_async_copy(sky_hbm, sky_all.at[det], sky_sem.at[0])

    def place_of(k):
        return partner(pair, k, n_pairs) if pushes else 0

    lead_sem = col_send.at[(bm + n_bm - 1) % n_bm]

    def fetch(k):
        pltpu.make_async_copy(
            wig_hbm.at[:, pl.ds(place_of(k) * part_units, part_units)],
            slab.at[bm, pl.ds(k * chunk_units, chunk_units)].reshape(cycles, part_units, ROWS, band),
            lead_sem if k == 1 else col_send.at[bm],
        ).start()

    def fetch_all():
        for k in range(2, chunks):
            fetch(k)
        pltpu.make_async_copy(
            beam_hbm, slab.at[bm, pl.ds(wig_units, beam_units)], col_send.at[bm]
        ).start()
        fetch(0)

    last = pair == n_pairs - 1

    @pl.when(jnp.logical_not(last))
    def _():
        if pushes:
            fetch(1)
        load.start()
        fetch_all()

    @pl.when(last)
    def _():
        load.start()

    barrier = pltpu.get_barrier_semaphore()

    def greet(semaphore, to_det, to_bm):
        pl.semaphore_signal(semaphore, inc=1, device_id=(to_det, to_bm), device_id_type=MESH)

    greet(barrier, buddy, bm)
    for z in range(1, n_bm):
        @pl.when(bm < z)
        def _():
            greet(barrier, 2 * pair + 1, z)
    for k in range(1, n_pairs):
        greet(barrier, 2 * ((pair + k) % n_pairs), bm)

    @pl.when(last)
    def _():
        if pushes:
            fetch(1)
        fetch_all()

    slab_units = wig_units + beam_units
    sent_units = slab_units - chunk_units

    def push_to(z, first=chunk_units, stop=slab_units):
        part = slab.at[bm, pl.ds(first, stop - first)]
        return pltpu.make_async_remote_copy(
            src_ref=part, dst_ref=part,
            send_sem=col_send.at[z], recv_sem=col_recv.at[bm],
            device_id=(det, z), device_id_type=MESH,
        )

    def early_to(z):
        return pltpu.make_async_remote_copy(
            src_ref=early.at[bm], dst_ref=early.at[bm],
            send_sem=col_send.at[z], recv_sem=col_recv.at[bm],
            device_id=(det, z), device_id_type=MESH,
        )

    def cube_to(z):
        return pltpu.make_async_remote_copy(
            src_ref=cube_all.at[bm], dst_ref=cube_all.at[bm],
            send_sem=col_send.at[z], recv_sem=col_recv.at[bm],
            device_id=(det, z), device_id_type=MESH,
        )

    def landing(buffer, z):
        return pltpu.make_async_remote_copy(
            src_ref=buffer, dst_ref=buffer,
            send_sem=col_send.at[z], recv_sem=col_recv.at[z],
            device_id=(det, z), device_id_type=MESH,
        )

    early_units = ROWS * LANES * 4 // (ROWS * band * 2)
    moved = slab.at[bm, pl.ds(0, sent_units + early_units)]

    @pl.when(jnp.logical_not(even))
    def _():
        pl.semaphore_wait(barrier, 1 + 2 * bm)
        greet(ok, buddy, bm)

    @pl.when(even)
    def _():
        pl.semaphore_wait(ok, 1)

    if pushes:
        yields = jnp.logical_not(even) & (pair == 0) & (bm == n_bm - 1)
        at_once = jnp.logical_not(yields) & pushed(role, n_bm, bm, 0)

    def share_lead():
        part = slab.at[bm, pl.ds(chunk_units, chunk_units)]
        pltpu.make_async_copy(part, part, lead_sem).wait()

        @pl.when(at_once)
        def _():
            push_to(0, chunk_units, 2 * chunk_units).start()

    if pushes:
        @pl.when(jnp.logical_not(last))
        def _():
            share_lead()

    load.wait()
    to_buddy = pltpu.make_async_remote_copy(
        src_ref=sky_all.at[det], dst_ref=sky_all.at[det],
        send_sem=sky_sem.at[0], recv_sem=sky_sem.at[2],
        device_id=(buddy, bm), device_id_type=MESH,
    )
    to_buddy.start()
    pltpu.make_async_copy(theta_hbm, index.at[0], col_recv.at[bm]).start()
    pltpu.make_async_copy(phi_hbm, index.at[1], col_recv.at[bm]).start()
    pltpu.make_async_copy(psi_hbm, index.at[2], col_recv.at[bm]).start()

    def share_sky():
        @pl.when(even)
        def _():
            pl.semaphore_wait(barrier, n_det - 1)
            greet(ok, buddy, bm)

        @pl.when(jnp.logical_not(even))
        def _():
            pl.semaphore_wait(ok, 1)

        for flip in range(n_det - 1, 1, -1):
            pltpu.make_async_remote_copy(
                src_ref=sky_all.at[det], dst_ref=sky_all.at[det],
                send_sem=sky_sem.at[0], recv_sem=sky_sem.at[1],
                device_id=(partner(det, flip, n_det), bm), device_id_type=MESH,
            ).start()

    lane = lax.broadcasted_iota(jnp.int32, (ROWS, LANES), 1)
    blocks = 2 * per_tile
    imag_row = (lane // (depth * per_tile)) % 2
    sin_column = (lane // pairs) % 2
    part = (imag_row + sin_column) % 2
    code = ((lane // depth) % per_tile * 2 + part) * pairs + lane % pairs
    sign = jnp.where((imag_row == 0) & (sin_column == 1), -1.0, 1.0)
    sign_column = jnp.where(sin_column == 1, -1.0, 1.0)

    def widen(z, first):
        for k in range(first, chunks):
            rows = pl.ds(pl.multiple_of(place_of(k) * part_units * ROWS, ROWS), part_units * ROWS)
            for g in range(cycles):
                block = slab[z, pl.ds(k * chunk_units + g * part_units, part_units)]
                wide[g, rows] = block.astype(F32).reshape(part_units * ROWS, band)

    def totals(z, sky, at):
        beam = slab[z, pl.ds(wig_units, beam_units)].astype(F32).reshape(beam_units * ROWS, band)
        for p in range(planes):
            re = im = 0.0
            for c in range(3):
                b0 = beam[c * planes + p : c * planes + p + 1]
                b1 = beam[(3 + c) * planes + p : (3 + c) * planes + p + 1]
                re = re + (sky[0][c] * b0 - sky[1][c] * b1)
                im = im + (sky[0][c] * b1 + sky[1][c] * b0)
            re = re.astype(BF16).astype(F32)
            im = im.astype(BF16).astype(F32)
            for g in range(cycles):
                w = wide[g, pl.ds(at * planes + p, ROWS, stride=planes)]
                for k, spectra in enumerate((re, im)):
                    yield k, g * planes + p, jnp.sum(w * spectra, axis=1, keepdims=True)

    shared = 2 * owned
    own_group = pair * shared // ROWS

    def send_early():
        to_buddy.wait_recv()
        near = [
            [
                sky_all[pl.ds(2 * pair, 2), r, c].astype(F32).reshape(shared, band)
                for c in range(3)
            ]
            for r in range(2)
        ]
        sky = [[jnp.concatenate([x] * (ROWS // shared), axis=0) for x in y] for y in near]
        packed = jnp.zeros((ROWS, LANES), F32)
        for k, i, total in totals(bm, sky, pl.multiple_of(own_group * ROWS, ROWS)):
            packed = jnp.where(part * pairs + lane % pairs == k * pairs + i, total, packed)
        early[bm] = packed * sign
        early_to(0).start()

    def share_slab():
        if pushes:
            @pl.when(last)
            def _():
                share_lead()

        rest = slab.at[bm, pl.ds(0, slab_units - chunk_units if pushes else slab_units)]
        pltpu.make_async_copy(rest, rest, col_send.at[bm]).wait()
        if pushes:
            @pl.when(at_once)
            def _():
                push_to(0, 2 * chunk_units).start()
        for z in range(n_bm - 1):
            @pl.when(bm > z)
            def _():
                greet(hello, det, z)
        widen(bm, 0)
        if pushes:
            @pl.when(pushed(role, n_bm, bm, 0))
            def _():
                send_early()

            @pl.when(yields & pushed(role, n_bm, bm, 0))
            def _():
                push_to(0).start()

    @pl.when(last)
    def _():
        share_sky()

    share_slab()

    @pl.when(jnp.logical_not(last))
    def _():
        share_sky()

    def share_inner(now):
        for z in range(1, n_bm - 1):
            @pl.when(now & pushed(role, n_bm, bm, z))
            def _():
                push_to(z).start()
                early_to(z).start()

    if pushes:
        share_inner((pair == 0) | jnp.logical_not(even))

    others = sky_all.at[pl.ds(0, n_det - 2)]
    skies = pltpu.make_async_remote_copy(
        src_ref=others, dst_ref=others,
        send_sem=sky_sem.at[0], recv_sem=sky_sem.at[1],
        device_id=(buddy, bm), device_id_type=MESH,
    )
    pltpu.make_async_copy(index, index, col_recv.at[bm]).wait()

    def mine(values):
        own = values[:, :width]
        for i in range(1, n_bm):
            own = jnp.where(bm == i, values[:, i * width : (i + 1) * width], own)
        return rows_of(own, groups, width)

    theta, phi, psi = mine(index[0]), mine(index[1]), mine(index[2])
    span = groups * width
    k_rows = n_bm * depth
    row = lax.broadcasted_iota(jnp.int32, (k_rows, span), 0)
    plane = row // depth * planes + row % planes
    cycle = (row // planes) % cycles
    quarter = ((row // pairs) % 2) * (3 * NPSI // 4)
    m_rows = 2 * modes
    mrow = lax.broadcasted_iota(jnp.int32, (m_rows, span), 0)
    mode = (mrow // (2 * tile_modes)) * tile_modes + mrow % tile_modes
    mquarter = ((mrow // tile_modes) % 2) * (NPHI // 4)
    for j in range(ROWS):
        at = pl.ds(j * span, span)
        step = (plane * psi[j : j + 1] + quarter) & (NPSI - 1)
        value = jnp.where(cycle == theta[j : j + 1], cos_on_grid(step, NPSI), 0.0)
        feat[:, at] = value.astype(BF16)
        step = (mode * phi[j : j + 1] + mquarter) & (NPHI - 1)
        phase[:, at] = cos_on_grid(step, NPHI)

    if pushes:
        share_inner((pair != 0) & even)

        @pl.when(jnp.logical_not(pushed(role, n_bm, bm, 0)))
        def _():
            to_buddy.wait_recv()
    else:
        to_buddy.wait_recv()
    skies.wait_recv()

    slots = tile_modes // owned
    for t in range(tiles):
        for r in range(2):
            for c in range(3):
                sky_wide[r, c, pl.ds(t * tile_modes, tile_modes)] = (
                    sky_all[t * slots : (t + 1) * slots, r, c].astype(F32).reshape(tile_modes, band)
                )

    def tile_totals(z, t, h):
        at = t * tile_modes + h * ROWS
        sky = [[sky_wide[r, c, pl.ds(at, ROWS)] for c in range(3)] for r in range(2)]
        return totals(z, sky, at)

    def profile(z):
        for t in range(tiles):
            packed = jnp.zeros((ROWS, LANES), F32)
            for h in range(per_tile):
                for k, i, total in tile_totals(z, t, h):
                    packed = jnp.where(code == (h * 2 + k) * pairs + i, total, packed)
            cube_all[z, t] = packed * sign

    def profile_here(z):
        inner = lane - z * depth
        inside = lane // depth == z
        for t in range(tiles):
            for h in range(per_tile):
                real = imag = jnp.zeros((ROWS, LANES), F32)
                for k, i, total in tile_totals(z, t, h):
                    cos_place, sin_place = inner == i, inner == pairs + i
                    real = jnp.where(sin_place if k else cos_place, total, real)
                    imag = jnp.where(cos_place if k else sin_place, total, imag)
                left[t, h] = jnp.where(inside, real * sign_column, left[t, h])
                left[t, per_tile + h] = jnp.where(inside, imag, left[t, per_tile + h])
        row = lax.broadcasted_iota(jnp.int32, (ROWS, LANES), 0)
        known = inside & (row // shared == pair % (ROWS // shared))
        for q in range(blocks):
            ready = pltpu.roll(early[z], (z - q) % n_bm * depth, 1)
            left[0, q] = jnp.where(known & (own_group == q % per_tile), ready, left[0, q])

    def place(z):
        inside = lane // depth == z
        for t in range(tiles):
            for q in range(blocks):
                moved = pltpu.roll(cube_all[z, t], (z - q) % n_bm * depth, 1)
                left[t, q] = jnp.where(inside, moved, left[t, q])

    profile(bm)

    @pl.when(bm < n_bm - 1)
    def _():
        pl.semaphore_wait(hello, n_bm - 1 - bm)

    def by_cube(source, target):
        apart = source != target
        return apart & jnp.logical_not(pushed(role, n_bm, source, target)) if pushes else apart

    for z in range(n_bm - 1, -1, -1):
        @pl.when(by_cube(bm, z))
        def _():
            cube_to(z).start()

    left[...] = jnp.zeros_like(left)
    for z in range(n_bm):
        @pl.when(bm == z)
        def _():
            place(z)

    def take(z):
        landing(moved, z).wait_recv()
        widen(z, 1)
        profile_here(z)

    def finish():
        wave = left[...].reshape(m_rows, k_rows)
        high = wave.astype(BF16)
        low = (wave - high.astype(F32)).astype(BF16)
        both = jnp.concatenate([high, low], axis=0)
        y = jnp.dot(both, feat[...], preferred_element_type=F32)
        terms = (y[:m_rows] + y[m_rows:]) * phase[...]
        total = jnp.sum(terms, axis=0, keepdims=True)
        for j in range(ROWS):
            for i in range(groups):
                at = j * span + i * width
                out_ref[pl.ds(i * ROWS + j, 1), :] = total[:, at : at + width]

    def finish_mixed():
        if pushes:
            for z in range(1, n_bm):
                @pl.when(pushed(role, n_bm, z, bm))
                def _():
                    take(z)
        for z in range(n_bm):
            @pl.when(by_cube(z, bm))
            def _():
                landing(cube_all.at[z], z).wait_recv()
                place(z)
        finish()

    if pushes:
        @pl.when(bm == 0)
        def _():
            for z in range(1, n_bm):
                take(z)
            finish()

        @pl.when(bm > 0)
        def _():
            finish_mixed()
    else:
        finish_mixed()

    every = sky_all.at[pl.ds(0, n_det - 1)]
    outbound = pltpu.make_async_remote_copy(
        src_ref=every, dst_ref=every,
        send_sem=sky_sem.at[0], recv_sem=sky_sem.at[1],
        device_id=(buddy, bm), device_id_type=MESH,
    )
    outbound.wait_send()
    for z in range(n_bm):
        @pl.when(by_cube(bm, z))
        def _():
            cube_to(z).wait_send()
        if pushes and z < n_bm - 1:
            @pl.when(pushed(role, n_bm, bm, z))
            def _():
                landing(moved, z).wait_send()


def on_device(sky_alm, beam_blm, wigner, theta_index, phi_index, psi_index):
    n_det, n_bm = lax.axis_size("det"), lax.axis_size("bm")
    cycles, modes, planes, band = wigner.shape
    dets, samples = theta_index.shape
    width = samples // n_bm
    span = dets // ROWS * width
    depth = 2 * cycles * planes
    tiles = modes * 2 * depth // (ROWS * LANES)
    beam_rows = 6 * planes
    units = modes * planes // ROWS
    wig_units = cycles * units
    beam_units = beam_rows // ROWS
    pushes = tiles == 1 and 2 * wig_units * ROWS * band <= PUSH_BYTES
    any_space = pl.BlockSpec(memory_space=pl.ANY)
    return pl.pallas_call(
        functools.partial(kernel, n_det, n_bm, modes, pushes),
        out_shape=pltpu.VMEM((dets, width), F32),
        in_specs=[any_space] * 6,
        out_specs=pl.BlockSpec(memory_space=pltpu.VMEM),
        scratch_shapes=[
            pltpu.VMEM((n_det, *sky_alm.shape), BF16),
            pltpu.VMEM((n_bm, wig_units + beam_units, ROWS, band), BF16),
            pltpu.VMEM((3, dets, samples), jnp.int32),
            pltpu.VMEM((2, 3, modes, band), F32),
            pltpu.VMEM((cycles, modes * planes, band), F32),
            pltpu.VMEM((n_bm * depth, ROWS * span), BF16),
            pltpu.VMEM((2 * modes, ROWS * span), F32),
            pltpu.VMEM((n_bm, tiles, ROWS, LANES), F32),
            pltpu.VMEM((n_bm, ROWS, LANES), F32),
            pltpu.VMEM((tiles, LANES // depth, ROWS, LANES), F32),
            pltpu.SemaphoreType.DMA((3,)),
            pltpu.SemaphoreType.DMA((n_bm,)),
            pltpu.SemaphoreType.DMA((n_bm,)),
            pltpu.SemaphoreType.REGULAR,
            pltpu.SemaphoreType.REGULAR,
        ],
        compiler_params=pltpu.CompilerParams(collective_id=0, has_side_effects=True),
    )(
        sky_alm,
        beam_blm.reshape(beam_units, ROWS, band),
        wigner.reshape(cycles, units, ROWS, band),
        theta_index,
        phi_index,
        psi_index,
    )


def solution(mesh):
    placed = (
        P(None, None, "det", None),
        P(None, None, "bm", None),
        P("det", None, "bm", None),
        P("det", None),
        P("det", None),
        P("det", None),
    )
    return jax.shard_map(
        on_device, mesh=mesh, in_specs=placed, out_specs=P("det", "bm"), check_vma=False
    )
```

```python
import functools
import math

import jax
import jax.numpy as jnp
from jax import lax
from jax.experimental import pallas as pl
from jax.experimental.pallas import tpu as pltpu
from jax.sharding import PartitionSpec as P

NPHI = 16384
NPSI = 32

TWO_PI = 2.0 * math.pi
LANES = 128
ROWS = 8
PUSH_BYTES = 1 << 18
F32 = jnp.float32
BF16 = jnp.bfloat16
MESH = pl.DeviceIdType.MESH


def cos_on_grid(step, grid):
    shift = (grid // 4).bit_length() - 1
    turn = (step + grid // 8) >> shift
    x = (step - (turn << shift)).astype(F32) * (TWO_PI / grid)
    x2 = x * x
    c = 1.0 + x2 * (-0.5 + x2 * (1 / 24 + x2 * (-1 / 720 + x2 * (1 / 40320))))
    s = x * (1.0 + x2 * (-1 / 6 + x2 * (1 / 120 + x2 * (-1 / 5040 + x2 * (1 / 362880)))))
    odd = (turn & 1) == 1
    value = jnp.where(odd, -s, c)
    return jnp.where((turn & 2) == 2, -value, value)


def partner(me, flip, n):
    out, bit = 0, 1
    while bit < n:
        digit = (me // bit) % 2
        out = out + bit * ((1 - digit) if flip & bit else digit)
        bit *= 2
    return out


def rows_of(values, groups, width):
    return jnp.concatenate([values[j * ROWS : (j + 1) * ROWS] for j in range(groups)], axis=1)


def pushed(role, n_bm, source, target):
    even, inner = role
    top = even & (source == n_bm - 1)
    return (source > target) & ((target == 0) | top | (inner & (source - target >= 2)))


def kernel(
    n_det, n_bm, modes, pushes,
    sky_hbm, beam_hbm, wig_hbm, theta_hbm, phi_hbm, psi_hbm, out_ref,
    sky_all, slab, index, sky_wide, wide, feat, phase, cube_all, early, left,
    sky_sem, col_send, col_recv, ok, hello,
):
    det = lax.axis_index("det")
    bm = lax.axis_index("bm")
    even = det % 2 == 0
    pair = det // 2
    buddy = det + 1 - 2 * (det % 2)
    n_pairs = n_det // 2
    role = even, even | (pair != n_pairs - 1)

    cycles, units, _, band = wig_hbm.shape
    beam_units = beam_hbm.shape[0]
    planes = beam_units * ROWS // 6
    owned = sky_all.shape[3]
    chunks = n_pairs if pushes else 1
    part_units = units // chunks
    chunk_units = cycles * part_units
    wig_units = cycles * units
    pairs = cycles * planes
    depth = 2 * pairs
    per_tile = LANES // (2 * depth)
    tile_modes = per_tile * ROWS
    tiles = modes // tile_modes
    dets, samples = index.shape[1:]
    width = samples // n_bm
    groups = dets // ROWS

    load = pltpu.make_async_copy(sky_hbm, sky_all.at[det], sky_sem.at[0])

    def place_of(k):
        return partner(pair, k, n_pairs) if pushes else 0

    lead_sem = col_send.at[(bm + n_bm - 1) % n_bm]

    def fetch(k):
        pltpu.make_async_copy(
            wig_hbm.at[:, pl.ds(place_of(k) * part_units, part_units)],
            slab.at[bm, pl.ds(k * chunk_units, chunk_units)].reshape(cycles, part_units, ROWS, band),
            lead_sem if k == 1 else col_send.at[bm],
        ).start()

    def fetch_all():
        for k in range(2, chunks):
            fetch(k)
        pltpu.make_async_copy(
            beam_hbm, slab.at[bm, pl.ds(wig_units, beam_units)], col_send.at[bm]
        ).start()
        fetch(0)

    last = pair == n_pairs - 1

    ahead = even & jnp.logical_not(last)

    @pl.when(ahead)
    def _():
        if pushes:
            fetch(1)
        load.start()
        fetch_all()

    @pl.when(jnp.logical_not(ahead))
    def _():
        load.start()


    barrier = pltpu.get_barrier_semaphore()

    def greet(semaphore, to_det, to_bm):
        pl.semaphore_signal(semaphore, inc=1, device_id=(to_det, to_bm), device_id_type=MESH)

    greet(barrier, buddy, bm)
    for z in range(1, n_bm):
        @pl.when(bm < z)
        def _():
            greet(barrier, 2 * pair + 1, z)
    for k in range(1, n_pairs):
        greet(barrier, 2 * ((pair + k) % n_pairs), bm)

    @pl.when(jnp.logical_not(ahead))
    def _():
        if pushes:
            fetch(1)
        fetch_all()

    slab_units = wig_units + beam_units
    sent_units = slab_units - chunk_units

    def push_to(z, first=chunk_units, stop=slab_units):
        part = slab.at[bm, pl.ds(first, stop - first)]
        return pltpu.make_async_remote_copy(
            src_ref=part, dst_ref=part,
            send_sem=col_send.at[z], recv_sem=col_recv.at[bm],
            device_id=(det, z), device_id_type=MESH,
        )

    def early_to(z):
        return pltpu.make_async_remote_copy(
            src_ref=early.at[bm], dst_ref=early.at[bm],
            send_sem=col_send.at[z], recv_sem=col_recv.at[bm],
            device_id=(det, z), device_id_type=MESH,
        )

    def cube_to(z):
        return pltpu.make_async_remote_copy(
            src_ref=cube_all.at[bm], dst_ref=cube_all.at[bm],
            send_sem=col_send.at[z], recv_sem=col_recv.at[bm],
            device_id=(det, z), device_id_type=MESH,
        )

    def landing(buffer, z):
        return pltpu.make_async_remote_copy(
            src_ref=buffer, dst_ref=buffer,
            send_sem=col_send.at[z], recv_sem=col_recv.at[z],
            device_id=(det, z), device_id_type=MESH,
        )

    early_units = ROWS * LANES * 4 // (ROWS * band * 2)
    moved = slab.at[bm, pl.ds(0, sent_units + early_units)]

    @pl.when(jnp.logical_not(even))
    def _():
        pl.semaphore_wait(barrier, 1 + 2 * bm)
        greet(ok, buddy, bm)

    @pl.when(even)
    def _():
        pl.semaphore_wait(ok, 1)

    if pushes:
        yields = jnp.logical_not(even) & (pair == 0) & (bm == n_bm - 1)
        at_once = jnp.logical_not(yields) & pushed(role, n_bm, bm, 0)

    def share_lead():
        part = slab.at[bm, pl.ds(chunk_units, chunk_units)]
        pltpu.make_async_copy(part, part, lead_sem).wait()

        @pl.when(at_once)
        def _():
            push_to(0, chunk_units, 2 * chunk_units).start()

    if pushes:
        @pl.when(ahead)
        def _():
            share_lead()

    load.wait()
    to_buddy = pltpu.make_async_remote_copy(
        src_ref=sky_all.at[det], dst_ref=sky_all.at[det],
        send_sem=sky_sem.at[0], recv_sem=sky_sem.at[2],
        device_id=(buddy, bm), device_id_type=MESH,
    )
    to_buddy.start()
    pltpu.make_async_copy(theta_hbm, index.at[0], col_recv.at[bm]).start()
    pltpu.make_async_copy(phi_hbm, index.at[1], col_recv.at[bm]).start()
    pltpu.make_async_copy(psi_hbm, index.at[2], col_recv.at[bm]).start()

    def share_sky():
        @pl.when(even)
        def _():
            pl.semaphore_wait(barrier, n_det - 1)
            greet(ok, buddy, bm)

        @pl.when(jnp.logical_not(even))
        def _():
            pl.semaphore_wait(ok, 1)

        for flip in range(n_det - 1, 1, -1):
            pltpu.make_async_remote_copy(
                src_ref=sky_all.at[det], dst_ref=sky_all.at[det],
                send_sem=sky_sem.at[0], recv_sem=sky_sem.at[1],
                device_id=(partner(det, flip, n_det), bm), device_id_type=MESH,
            ).start()

    lane = lax.broadcasted_iota(jnp.int32, (ROWS, LANES), 1)
    blocks = 2 * per_tile
    imag_row = (lane // (depth * per_tile)) % 2
    sin_column = (lane // pairs) % 2
    part = (imag_row + sin_column) % 2
    code = ((lane // depth) % per_tile * 2 + part) * pairs + lane % pairs
    sign = jnp.where((imag_row == 0) & (sin_column == 1), -1.0, 1.0)
    sign_column = jnp.where(sin_column == 1, -1.0, 1.0)

    def widen(z, first):
        for k in range(first, chunks):
            rows = pl.ds(pl.multiple_of(place_of(k) * part_units * ROWS, ROWS), part_units * ROWS)
            for g in range(cycles):
                block = slab[z, pl.ds(k * chunk_units + g * part_units, part_units)]
                wide[g, rows] = block.astype(F32).reshape(part_units * ROWS, band)

    def totals(z, sky, at):
        beam = slab[z, pl.ds(wig_units, beam_units)].astype(F32).reshape(beam_units * ROWS, band)
        for p in range(planes):
            re = im = 0.0
            for c in range(3):
                b0 = beam[c * planes + p : c * planes + p + 1]
                b1 = beam[(3 + c) * planes + p : (3 + c) * planes + p + 1]
                re = re + (sky[0][c] * b0 - sky[1][c] * b1)
                im = im + (sky[0][c] * b1 + sky[1][c] * b0)
            re = re.astype(BF16).astype(F32)
            im = im.astype(BF16).astype(F32)
            for g in range(cycles):
                w = wide[g, pl.ds(at * planes + p, ROWS, stride=planes)]
                for k, spectra in enumerate((re, im)):
                    yield k, g * planes + p, jnp.sum(w * spectra, axis=1, keepdims=True)

    shared = 2 * owned
    own_group = pair * shared // ROWS

    def send_early():
        to_buddy.wait_recv()
        near = [
            [
                sky_all[pl.ds(2 * pair, 2), r, c].astype(F32).reshape(shared, band)
                for c in range(3)
            ]
            for r in range(2)
        ]
        sky = [[jnp.concatenate([x] * (ROWS // shared), axis=0) for x in y] for y in near]
        packed = jnp.zeros((ROWS, LANES), F32)
        for k, i, total in totals(bm, sky, pl.multiple_of(own_group * ROWS, ROWS)):
            packed = jnp.where(part * pairs + lane % pairs == k * pairs + i, total, packed)
        early[bm] = packed * sign
        early_to(0).start()

    def share_slab():
        if pushes:
            @pl.when(jnp.logical_not(ahead))
            def _():
                share_lead()

        rest = slab.at[bm, pl.ds(0, slab_units - chunk_units if pushes else slab_units)]
        pltpu.make_async_copy(rest, rest, col_send.at[bm]).wait()
        if pushes:
            @pl.when(at_once)
            def _():
                push_to(0, 2 * chunk_units).start()
        for z in range(n_bm - 1):
            @pl.when(bm > z)
            def _():
                greet(hello, det, z)
        widen(bm, 0)
        if pushes:
            @pl.when(pushed(role, n_bm, bm, 0))
            def _():
                send_early()

            @pl.when(yields & pushed(role, n_bm, bm, 0))
            def _():
                push_to(0).start()

    @pl.when(last)
    def _():
        share_sky()

    share_slab()

    @pl.when(jnp.logical_not(last))
    def _():
        share_sky()

    def share_inner(now):
        for z in range(1, n_bm - 1):
            @pl.when(now & pushed(role, n_bm, bm, z))
            def _():
                push_to(z).start()
                early_to(z).start()

    if pushes:
        share_inner((pair == 0) | jnp.logical_not(even))

    others = sky_all.at[pl.ds(0, n_det - 2)]
    skies = pltpu.make_async_remote_copy(
        src_ref=others, dst_ref=others,
        send_sem=sky_sem.at[0], recv_sem=sky_sem.at[1],
        device_id=(buddy, bm), device_id_type=MESH,
    )
    pltpu.make_async_copy(index, index, col_recv.at[bm]).wait()

    def mine(values):
        own = values[:, :width]
        for i in range(1, n_bm):
            own = jnp.where(bm == i, values[:, i * width : (i + 1) * width], own)
        return rows_of(own, groups, width)

    theta, phi, psi = mine(index[0]), mine(index[1]), mine(index[2])
    span = groups * width
    k_rows = n_bm * depth
    row = lax.broadcasted_iota(jnp.int32, (k_rows, span), 0)
    plane = row // depth * planes + row % planes
    cycle = (row // planes) % cycles
    quarter = ((row // pairs) % 2) * (3 * NPSI // 4)
    m_rows = 2 * modes
    mrow = lax.broadcasted_iota(jnp.int32, (m_rows, span), 0)
    mode = (mrow // (2 * tile_modes)) * tile_modes + mrow % tile_modes
    mquarter = ((mrow // tile_modes) % 2) * (NPHI // 4)
    for j in range(ROWS):
        at = pl.ds(j * span, span)
        step = (plane * psi[j : j + 1] + quarter) & (NPSI - 1)
        value = jnp.where(cycle == theta[j : j + 1], cos_on_grid(step, NPSI), 0.0)
        feat[:, at] = value.astype(BF16)
        step = (mode * phi[j : j + 1] + mquarter) & (NPHI - 1)
        phase[:, at] = cos_on_grid(step, NPHI)

    if pushes:
        share_inner((pair != 0) & even)

        @pl.when(jnp.logical_not(pushed(role, n_bm, bm, 0)))
        def _():
            to_buddy.wait_recv()
    else:
        to_buddy.wait_recv()
    skies.wait_recv()

    slots = tile_modes // owned
    for t in range(tiles):
        for r in range(2):
            for c in range(3):
                sky_wide[r, c, pl.ds(t * tile_modes, tile_modes)] = (
                    sky_all[t * slots : (t + 1) * slots, r, c].astype(F32).reshape(tile_modes, band)
                )

    def tile_totals(z, t, h):
        at = t * tile_modes + h * ROWS
        sky = [[sky_wide[r, c, pl.ds(at, ROWS)] for c in range(3)] for r in range(2)]
        return totals(z, sky, at)

    def profile(z):
        for t in range(tiles):
            packed = jnp.zeros((ROWS, LANES), F32)
            for h in range(per_tile):
                for k, i, total in tile_totals(z, t, h):
                    packed = jnp.where(code == (h * 2 + k) * pairs + i, total, packed)
            cube_all[z, t] = packed * sign

    def profile_here(z):
        inner = lane - z * depth
        inside = lane // depth == z
        for t in range(tiles):
            for h in range(per_tile):
                real = imag = jnp.zeros((ROWS, LANES), F32)
                for k, i, total in tile_totals(z, t, h):
                    cos_place, sin_place = inner == i, inner == pairs + i
                    real = jnp.where(sin_place if k else cos_place, total, real)
                    imag = jnp.where(cos_place if k else sin_place, total, imag)
                left[t, h] = jnp.where(inside, real * sign_column, left[t, h])
                left[t, per_tile + h] = jnp.where(inside, imag, left[t, per_tile + h])
        row = lax.broadcasted_iota(jnp.int32, (ROWS, LANES), 0)
        known = inside & (row // shared == pair % (ROWS // shared))
        for q in range(blocks):
            ready = pltpu.roll(early[z], (z - q) % n_bm * depth, 1)
            left[0, q] = jnp.where(known & (own_group == q % per_tile), ready, left[0, q])

    def place(z):
        inside = lane // depth == z
        for t in range(tiles):
            for q in range(blocks):
                moved = pltpu.roll(cube_all[z, t], (z - q) % n_bm * depth, 1)
                left[t, q] = jnp.where(inside, moved, left[t, q])

    profile(bm)

    @pl.when(bm < n_bm - 1)
    def _():
        pl.semaphore_wait(hello, n_bm - 1 - bm)

    def by_cube(source, target):
        apart = source != target
        return apart & jnp.logical_not(pushed(role, n_bm, source, target)) if pushes else apart

    for z in range(n_bm - 1, -1, -1):
        @pl.when(by_cube(bm, z))
        def _():
            cube_to(z).start()

    left[...] = jnp.zeros_like(left)
    for z in range(n_bm):
        @pl.when(bm == z)
        def _():
            place(z)

    def take(z):
        landing(moved, z).wait_recv()
        widen(z, 1)
        profile_here(z)

    def finish():
        wave = left[...].reshape(m_rows, k_rows)
        high = wave.astype(BF16)
        low = (wave - high.astype(F32)).astype(BF16)
        both = jnp.concatenate([high, low], axis=0)
        y = jnp.dot(both, feat[...], preferred_element_type=F32)
        terms = (y[:m_rows] + y[m_rows:]) * phase[...]
        total = jnp.sum(terms, axis=0, keepdims=True)
        for j in range(ROWS):
            for i in range(groups):
                at = j * span + i * width
                out_ref[pl.ds(i * ROWS + j, 1), :] = total[:, at : at + width]

    def finish_mixed():
        if pushes:
            for z in range(1, n_bm):
                @pl.when(pushed(role, n_bm, z, bm))
                def _():
                    take(z)
        for z in range(n_bm):
            @pl.when(by_cube(z, bm))
            def _():
                landing(cube_all.at[z], z).wait_recv()
                place(z)
        finish()

    if pushes:
        @pl.when(bm == 0)
        def _():
            for z in range(1, n_bm):
                take(z)
            finish()

        @pl.when(bm > 0)
        def _():
            finish_mixed()
    else:
        finish_mixed()

    every = sky_all.at[pl.ds(0, n_det - 1)]
    outbound = pltpu.make_async_remote_copy(
        src_ref=every, dst_ref=every,
        send_sem=sky_sem.at[0], recv_sem=sky_sem.at[1],
        device_id=(buddy, bm), device_id_type=MESH,
    )
    outbound.wait_send()
    for z in range(n_bm):
        @pl.when(by_cube(bm, z))
        def _():
            cube_to(z).wait_send()
        if pushes and z < n_bm - 1:
            @pl.when(pushed(role, n_bm, bm, z))
            def _():
                landing(moved, z).wait_send()


def on_device(sky_alm, beam_blm, wigner, theta_index, phi_index, psi_index):
    n_det, n_bm = lax.axis_size("det"), lax.axis_size("bm")
    cycles, modes, planes, band = wigner.shape
    dets, samples = theta_index.shape
    width = samples // n_bm
    span = dets // ROWS * width
    depth = 2 * cycles * planes
    tiles = modes * 2 * depth // (ROWS * LANES)
    beam_rows = 6 * planes
    units = modes * planes // ROWS
    wig_units = cycles * units
    beam_units = beam_rows // ROWS
    pushes = tiles == 1 and 2 * wig_units * ROWS * band <= PUSH_BYTES
    any_space = pl.BlockSpec(memory_space=pl.ANY)
    return pl.pallas_call(
        functools.partial(kernel, n_det, n_bm, modes, pushes),
        out_shape=pltpu.VMEM((dets, width), F32),
        in_specs=[any_space] * 6,
        out_specs=pl.BlockSpec(memory_space=pltpu.VMEM),
        scratch_shapes=[
            pltpu.VMEM((n_det, *sky_alm.shape), BF16),
            pltpu.VMEM((n_bm, wig_units + beam_units, ROWS, band), BF16),
            pltpu.VMEM((3, dets, samples), jnp.int32),
            pltpu.VMEM((2, 3, modes, band), F32),
            pltpu.VMEM((cycles, modes * planes, band), F32),
            pltpu.VMEM((n_bm * depth, ROWS * span), BF16),
            pltpu.VMEM((2 * modes, ROWS * span), F32),
            pltpu.VMEM((n_bm, tiles, ROWS, LANES), F32),
            pltpu.VMEM((n_bm, ROWS, LANES), F32),
            pltpu.VMEM((tiles, LANES // depth, ROWS, LANES), F32),
            pltpu.SemaphoreType.DMA((3,)),
            pltpu.SemaphoreType.DMA((n_bm,)),
            pltpu.SemaphoreType.DMA((n_bm,)),
            pltpu.SemaphoreType.REGULAR,
            pltpu.SemaphoreType.REGULAR,
        ],
        compiler_params=pltpu.CompilerParams(collective_id=0, has_side_effects=True),
    )(
        sky_alm,
        beam_blm.reshape(beam_units, ROWS, band),
        wigner.reshape(cycles, units, ROWS, band),
        theta_index,
        phi_index,
        psi_index,
    )


def solution(mesh):
    placed = (
        P(None, None, "det", None),
        P(None, None, "bm", None),
        P("det", None, "bm", None),
        P("det", None),
        P("det", None),
        P("det", None),
    )
    return jax.shard_map(
        on_device, mesh=mesh, in_specs=placed, out_specs=P("det", "bm"), check_vma=False
    )
```

```python
import functools
import math

import jax
import jax.numpy as jnp
from jax import lax
from jax.experimental import pallas as pl
from jax.experimental.pallas import tpu as pltpu
from jax.sharding import PartitionSpec as P

NPHI = 16384
NPSI = 32

TWO_PI = 2.0 * math.pi
LANES = 128
ROWS = 8
PUSH_BYTES = 1 << 18
F32 = jnp.float32
BF16 = jnp.bfloat16
MESH = pl.DeviceIdType.MESH


def cos_on_grid(step, grid):
    shift = (grid // 4).bit_length() - 1
    turn = (step + grid // 8) >> shift
    x = (step - (turn << shift)).astype(F32) * (TWO_PI / grid)
    x2 = x * x
    c = 1.0 + x2 * (-0.5 + x2 * (1 / 24 + x2 * (-1 / 720 + x2 * (1 / 40320))))
    s = x * (1.0 + x2 * (-1 / 6 + x2 * (1 / 120 + x2 * (-1 / 5040 + x2 * (1 / 362880)))))
    odd = (turn & 1) == 1
    value = jnp.where(odd, -s, c)
    return jnp.where((turn & 2) == 2, -value, value)


def partner(me, flip, n):
    out, bit = 0, 1
    while bit < n:
        digit = (me // bit) % 2
        out = out + bit * ((1 - digit) if flip & bit else digit)
        bit *= 2
    return out


def rows_of(values, groups, width):
    return jnp.concatenate([values[j * ROWS : (j + 1) * ROWS] for j in range(groups)], axis=1)


def pushed(role, n_bm, source, target):
    even, inner = role
    top = even & (source == n_bm - 1)
    return (source > target) & ((target == 0) | top | (inner & (source - target >= 2)))


def kernel(
    n_det, n_bm, modes, pushes,
    sky_hbm, beam_hbm, wig_hbm, theta_hbm, phi_hbm, psi_hbm, out_ref,
    sky_all, slab, index, sky_wide, wide, feat, phase, cube_all, early, left,
    sky_sem, col_send, col_recv, ok, hello,
):
    det = lax.axis_index("det")
    bm = lax.axis_index("bm")
    even = det % 2 == 0
    pair = det // 2
    buddy = det + 1 - 2 * (det % 2)
    n_pairs = n_det // 2
    role = even, even | (pair != n_pairs - 1)

    cycles, units, _, band = wig_hbm.shape
    beam_units = beam_hbm.shape[0]
    planes = beam_units * ROWS // 6
    owned = sky_all.shape[3]
    chunks = n_pairs if pushes else 1
    part_units = units // chunks
    chunk_units = cycles * part_units
    wig_units = cycles * units
    pairs = cycles * planes
    depth = 2 * pairs
    per_tile = LANES // (2 * depth)
    tile_modes = per_tile * ROWS
    tiles = modes // tile_modes
    dets, samples = index.shape[1:]
    width = samples // n_bm
    groups = dets // ROWS

    load = pltpu.make_async_copy(sky_hbm, sky_all.at[det], sky_sem.at[0])

    def place_of(k):
        return partner(pair, k, n_pairs) if pushes else 0

    lead_sem = col_send.at[(bm + n_bm - 1) % n_bm]

    def fetch(k):
        pltpu.make_async_copy(
            wig_hbm.at[:, pl.ds(place_of(k) * part_units, part_units)],
            slab.at[bm, pl.ds(k * chunk_units, chunk_units)].reshape(cycles, part_units, ROWS, band),
            lead_sem if k == 1 else col_send.at[bm],
        ).start()

    def fetch_all():
        for k in range(2, chunks):
            fetch(k)
        pltpu.make_async_copy(
            beam_hbm, slab.at[bm, pl.ds(wig_units, beam_units)], col_send.at[bm]
        ).start()
        fetch(0)

    last = pair == n_pairs - 1

    ahead = even & jnp.logical_not(last)

    @pl.when(ahead)
    def _():
        if pushes:
            fetch(1)
        load.start()
        fetch_all()

    @pl.when(jnp.logical_not(ahead))
    def _():
        load.start()


    barrier = pltpu.get_barrier_semaphore()

    def greet(semaphore, to_det, to_bm):
        pl.semaphore_signal(semaphore, inc=1, device_id=(to_det, to_bm), device_id_type=MESH)

    greet(barrier, buddy, bm)
    for z in range(1, n_bm):
        @pl.when(bm < z)
        def _():
            greet(barrier, 2 * pair + 1, z)
    for k in range(1, n_pairs):
        greet(barrier, 2 * ((pair + k) % n_pairs), bm)

    @pl.when(jnp.logical_not(ahead))
    def _():
        if pushes:
            fetch(1)
        fetch_all()

    slab_units = wig_units + beam_units
    sent_units = slab_units - chunk_units

    def push_to(z, first=chunk_units, stop=slab_units):
        part = slab.at[bm, pl.ds(first, stop - first)]
        return pltpu.make_async_remote_copy(
            src_ref=part, dst_ref=part,
            send_sem=col_send.at[z], recv_sem=col_recv.at[bm],
            device_id=(det, z), device_id_type=MESH,
        )

    def early_to(z):
        return pltpu.make_async_remote_copy(
            src_ref=early.at[bm], dst_ref=early.at[bm],
            send_sem=col_send.at[z], recv_sem=col_recv.at[bm],
            device_id=(det, z), device_id_type=MESH,
        )

    def cube_to(z):
        return pltpu.make_async_remote_copy(
            src_ref=cube_all.at[bm], dst_ref=cube_all.at[bm],
            send_sem=col_send.at[z], recv_sem=col_recv.at[bm],
            device_id=(det, z), device_id_type=MESH,
        )

    def landing(buffer, z):
        return pltpu.make_async_remote_copy(
            src_ref=buffer, dst_ref=buffer,
            send_sem=col_send.at[z], recv_sem=col_recv.at[z],
            device_id=(det, z), device_id_type=MESH,
        )

    early_units = ROWS * LANES * 4 // (ROWS * band * 2)
    moved = slab.at[bm, pl.ds(0, sent_units + early_units)]

    @pl.when(jnp.logical_not(even))
    def _():
        pl.semaphore_wait(barrier, 1 + 2 * bm)
        greet(ok, buddy, bm)

    @pl.when(even)
    def _():
        pl.semaphore_wait(ok, 1)

    if pushes:
        yields = jnp.logical_not(even) & (pair == 0) & (bm == n_bm - 1)
        at_once = jnp.logical_not(yields) & pushed(role, n_bm, bm, 0)

    def share_lead():
        part = slab.at[bm, pl.ds(chunk_units, chunk_units)]
        pltpu.make_async_copy(part, part, lead_sem).wait()

        @pl.when(at_once)
        def _():
            push_to(0, chunk_units, 2 * chunk_units).start()

    if pushes:
        @pl.when(ahead)
        def _():
            share_lead()

    load.wait()
    to_buddy = pltpu.make_async_remote_copy(
        src_ref=sky_all.at[det], dst_ref=sky_all.at[det],
        send_sem=sky_sem.at[0], recv_sem=sky_sem.at[2],
        device_id=(buddy, bm), device_id_type=MESH,
    )
    to_buddy.start()
    pltpu.make_async_copy(theta_hbm, index.at[0], col_recv.at[bm]).start()
    pltpu.make_async_copy(phi_hbm, index.at[1], col_recv.at[bm]).start()
    pltpu.make_async_copy(psi_hbm, index.at[2], col_recv.at[bm]).start()

    def share_sky():
        @pl.when(even)
        def _():
            pl.semaphore_wait(barrier, n_det - 1)
            greet(ok, buddy, bm)

        @pl.when(jnp.logical_not(even))
        def _():
            pl.semaphore_wait(ok, 1)

        for flip in range(n_det - 1, 1, -1):
            pltpu.make_async_remote_copy(
                src_ref=sky_all.at[det], dst_ref=sky_all.at[det],
                send_sem=sky_sem.at[0], recv_sem=sky_sem.at[1],
                device_id=(partner(det, flip, n_det), bm), device_id_type=MESH,
            ).start()

    lane = lax.broadcasted_iota(jnp.int32, (ROWS, LANES), 1)
    blocks = 2 * per_tile
    imag_row = (lane // (depth * per_tile)) % 2
    sin_column = (lane // pairs) % 2
    part = (imag_row + sin_column) % 2
    code = ((lane // depth) % per_tile * 2 + part) * pairs + lane % pairs
    sign = jnp.where((imag_row == 0) & (sin_column == 1), -1.0, 1.0)
    sign_column = jnp.where(sin_column == 1, -1.0, 1.0)

    def widen(z, first, stop=chunks):
        for k in range(first, stop):
            rows = pl.ds(pl.multiple_of(place_of(k) * part_units * ROWS, ROWS), part_units * ROWS)
            for g in range(cycles):
                block = slab[z, pl.ds(k * chunk_units + g * part_units, part_units)]
                wide[g, rows] = block.astype(F32).reshape(part_units * ROWS, band)

    def totals(z, sky, at):
        beam = slab[z, pl.ds(wig_units, beam_units)].astype(F32).reshape(beam_units * ROWS, band)
        for p in range(planes):
            re = im = 0.0
            for c in range(3):
                b0 = beam[c * planes + p : c * planes + p + 1]
                b1 = beam[(3 + c) * planes + p : (3 + c) * planes + p + 1]
                re = re + (sky[0][c] * b0 - sky[1][c] * b1)
                im = im + (sky[0][c] * b1 + sky[1][c] * b0)
            re = re.astype(BF16).astype(F32)
            im = im.astype(BF16).astype(F32)
            for g in range(cycles):
                w = wide[g, pl.ds(at * planes + p, ROWS, stride=planes)]
                for k, spectra in enumerate((re, im)):
                    yield k, g * planes + p, jnp.sum(w * spectra, axis=1, keepdims=True)

    shared = 2 * owned
    own_group = pair * shared // ROWS

    def send_early():
        to_buddy.wait_recv()
        near = [
            [
                sky_all[pl.ds(2 * pair, 2), r, c].astype(F32).reshape(shared, band)
                for c in range(3)
            ]
            for r in range(2)
        ]
        sky = [[jnp.concatenate([x] * (ROWS // shared), axis=0) for x in y] for y in near]
        packed = jnp.zeros((ROWS, LANES), F32)
        for k, i, total in totals(bm, sky, pl.multiple_of(own_group * ROWS, ROWS)):
            packed = jnp.where(part * pairs + lane % pairs == k * pairs + i, total, packed)
        early[bm] = packed * sign
        early_to(0).start()

    near_chunks = min(chunks, max(1, ROWS // (2 * sky_all.shape[3]))) if pushes else chunks

    def share_slab():
        if pushes:
            @pl.when(jnp.logical_not(ahead))
            def _():
                share_lead()

        rest = slab.at[bm, pl.ds(0, slab_units - chunk_units if pushes else slab_units)]
        pltpu.make_async_copy(rest, rest, col_send.at[bm]).wait()
        if pushes:
            @pl.when(at_once)
            def _():
                push_to(0, 2 * chunk_units).start()
        for z in range(n_bm - 1):
            @pl.when(bm > z)
            def _():
                greet(hello, det, z)
        widen(bm, 0, near_chunks)
        if pushes:
            @pl.when(pushed(role, n_bm, bm, 0))
            def _():
                send_early()

            @pl.when(yields & pushed(role, n_bm, bm, 0))
            def _():
                push_to(0).start()

        widen(bm, near_chunks)

    @pl.when(last)
    def _():
        share_sky()

    share_slab()

    @pl.when(jnp.logical_not(last))
    def _():
        share_sky()

    def share_inner(now):
        for z in range(1, n_bm - 1):
            @pl.when(now & pushed(role, n_bm, bm, z))
            def _():
                push_to(z).start()
                early_to(z).start()

    if pushes:
        share_inner((pair == 0) | jnp.logical_not(even))

    others = sky_all.at[pl.ds(0, n_det - 2)]
    skies = pltpu.make_async_remote_copy(
        src_ref=others, dst_ref=others,
        send_sem=sky_sem.at[0], recv_sem=sky_sem.at[1],
        device_id=(buddy, bm), device_id_type=MESH,
    )
    pltpu.make_async_copy(index, index, col_recv.at[bm]).wait()

    def mine(values):
        own = values[:, :width]
        for i in range(1, n_bm):
            own = jnp.where(bm == i, values[:, i * width : (i + 1) * width], own)
        return rows_of(own, groups, width)

    theta, phi, psi = mine(index[0]), mine(index[1]), mine(index[2])
    span = groups * width
    k_rows = n_bm * depth
    row = lax.broadcasted_iota(jnp.int32, (k_rows, span), 0)
    plane = row // depth * planes + row % planes
    cycle = (row // planes) % cycles
    quarter = ((row // pairs) % 2) * (3 * NPSI // 4)
    m_rows = 2 * modes
    mrow = lax.broadcasted_iota(jnp.int32, (m_rows, span), 0)
    mode = (mrow // (2 * tile_modes)) * tile_modes + mrow % tile_modes
    mquarter = ((mrow // tile_modes) % 2) * (NPHI // 4)
    for j in range(ROWS):
        at = pl.ds(j * span, span)
        step = (plane * psi[j : j + 1] + quarter) & (NPSI - 1)
        value = jnp.where(cycle == theta[j : j + 1], cos_on_grid(step, NPSI), 0.0)
        feat[:, at] = value.astype(BF16)
        step = (mode * phi[j : j + 1] + mquarter) & (NPHI - 1)
        phase[:, at] = cos_on_grid(step, NPHI)

    if pushes:
        share_inner((pair != 0) & even)

        @pl.when(jnp.logical_not(pushed(role, n_bm, bm, 0)))
        def _():
            to_buddy.wait_recv()
    else:
        to_buddy.wait_recv()
    skies.wait_recv()

    slots = tile_modes // owned
    for t in range(tiles):
        for r in range(2):
            for c in range(3):
                sky_wide[r, c, pl.ds(t * tile_modes, tile_modes)] = (
                    sky_all[t * slots : (t + 1) * slots, r, c].astype(F32).reshape(tile_modes, band)
                )

    def tile_totals(z, t, h):
        at = t * tile_modes + h * ROWS
        sky = [[sky_wide[r, c, pl.ds(at, ROWS)] for c in range(3)] for r in range(2)]
        return totals(z, sky, at)

    def profile(z):
        for t in range(tiles):
            packed = jnp.zeros((ROWS, LANES), F32)
            for h in range(per_tile):
                for k, i, total in tile_totals(z, t, h):
                    packed = jnp.where(code == (h * 2 + k) * pairs + i, total, packed)
            cube_all[z, t] = packed * sign

    def profile_here(z):
        inner = lane - z * depth
        inside = lane // depth == z
        for t in range(tiles):
            for h in range(per_tile):
                real = imag = jnp.zeros((ROWS, LANES), F32)
                for k, i, total in tile_totals(z, t, h):
                    cos_place, sin_place = inner == i, inner == pairs + i
                    real = jnp.where(sin_place if k else cos_place, total, real)
                    imag = jnp.where(cos_place if k else sin_place, total, imag)
                left[t, h] = jnp.where(inside, real * sign_column, left[t, h])
                left[t, per_tile + h] = jnp.where(inside, imag, left[t, per_tile + h])
        row = lax.broadcasted_iota(jnp.int32, (ROWS, LANES), 0)
        known = inside & (row // shared == pair % (ROWS // shared))
        for q in range(blocks):
            ready = pltpu.roll(early[z], (z - q) % n_bm * depth, 1)
            left[0, q] = jnp.where(known & (own_group == q % per_tile), ready, left[0, q])

    def place(z):
        inside = lane // depth == z
        for t in range(tiles):
            for q in range(blocks):
                moved = pltpu.roll(cube_all[z, t], (z - q) % n_bm * depth, 1)
                left[t, q] = jnp.where(inside, moved, left[t, q])

    profile(bm)

    @pl.when(bm < n_bm - 1)
    def _():
        pl.semaphore_wait(hello, n_bm - 1 - bm)

    def by_cube(source, target):
        apart = source != target
        return apart & jnp.logical_not(pushed(role, n_bm, source, target)) if pushes else apart

    for z in range(n_bm - 1, -1, -1):
        @pl.when(by_cube(bm, z))
        def _():
            cube_to(z).start()

    left[...] = jnp.zeros_like(left)
    for z in range(n_bm):
        @pl.when(bm == z)
        def _():
            place(z)

    def take(z):
        landing(moved, z).wait_recv()
        widen(z, 1)
        profile_here(z)

    def finish():
        wave = left[...].reshape(m_rows, k_rows)
        high = wave.astype(BF16)
        low = (wave - high.astype(F32)).astype(BF16)
        both = jnp.concatenate([high, low], axis=0)
        y = jnp.dot(both, feat[...], preferred_element_type=F32)
        terms = (y[:m_rows] + y[m_rows:]) * phase[...]
        total = jnp.sum(terms, axis=0, keepdims=True)
        for j in range(ROWS):
            for i in range(groups):
                at = j * span + i * width
                out_ref[pl.ds(i * ROWS + j, 1), :] = total[:, at : at + width]

    def finish_mixed():
        if pushes:
            for z in range(1, n_bm):
                @pl.when(pushed(role, n_bm, z, bm))
                def _():
                    take(z)
        for z in range(n_bm):
            @pl.when(by_cube(z, bm))
            def _():
                landing(cube_all.at[z], z).wait_recv()
                place(z)
        finish()

    if pushes:
        @pl.when(bm == 0)
        def _():
            for z in range(1, n_bm):
                take(z)
            finish()

        @pl.when(bm > 0)
        def _():
            finish_mixed()
    else:
        finish_mixed()

    every = sky_all.at[pl.ds(0, n_det - 1)]
    outbound = pltpu.make_async_remote_copy(
        src_ref=every, dst_ref=every,
        send_sem=sky_sem.at[0], recv_sem=sky_sem.at[1],
        device_id=(buddy, bm), device_id_type=MESH,
    )
    outbound.wait_send()
    for z in range(n_bm):
        @pl.when(by_cube(bm, z))
        def _():
            cube_to(z).wait_send()
        if pushes and z < n_bm - 1:
            @pl.when(pushed(role, n_bm, bm, z))
            def _():
                landing(moved, z).wait_send()


def on_device(sky_alm, beam_blm, wigner, theta_index, phi_index, psi_index):
    n_det, n_bm = lax.axis_size("det"), lax.axis_size("bm")
    cycles, modes, planes, band = wigner.shape
    dets, samples = theta_index.shape
    width = samples // n_bm
    span = dets // ROWS * width
    depth = 2 * cycles * planes
    tiles = modes * 2 * depth // (ROWS * LANES)
    beam_rows = 6 * planes
    units = modes * planes // ROWS
    wig_units = cycles * units
    beam_units = beam_rows // ROWS
    pushes = tiles == 1 and 2 * wig_units * ROWS * band <= PUSH_BYTES
    any_space = pl.BlockSpec(memory_space=pl.ANY)
    return pl.pallas_call(
        functools.partial(kernel, n_det, n_bm, modes, pushes),
        out_shape=pltpu.VMEM((dets, width), F32),
        in_specs=[any_space] * 6,
        out_specs=pl.BlockSpec(memory_space=pltpu.VMEM),
        scratch_shapes=[
            pltpu.VMEM((n_det, *sky_alm.shape), BF16),
            pltpu.VMEM((n_bm, wig_units + beam_units, ROWS, band), BF16),
            pltpu.VMEM((3, dets, samples), jnp.int32),
            pltpu.VMEM((2, 3, modes, band), F32),
            pltpu.VMEM((cycles, modes * planes, band), F32),
            pltpu.VMEM((n_bm * depth, ROWS * span), BF16),
            pltpu.VMEM((2 * modes, ROWS * span), F32),
            pltpu.VMEM((n_bm, tiles, ROWS, LANES), F32),
            pltpu.VMEM((n_bm, ROWS, LANES), F32),
            pltpu.VMEM((tiles, LANES // depth, ROWS, LANES), F32),
            pltpu.SemaphoreType.DMA((3,)),
            pltpu.SemaphoreType.DMA((n_bm,)),
            pltpu.SemaphoreType.DMA((n_bm,)),
            pltpu.SemaphoreType.REGULAR,
            pltpu.SemaphoreType.REGULAR,
        ],
        compiler_params=pltpu.CompilerParams(collective_id=0, has_side_effects=True),
    )(
        sky_alm,
        beam_blm.reshape(beam_units, ROWS, band),
        wigner.reshape(cycles, units, ROWS, band),
        theta_index,
        phi_index,
        psi_index,
    )


def solution(mesh):
    placed = (
        P(None, None, "det", None),
        P(None, None, "bm", None),
        P("det", None, "bm", None),
        P("det", None),
        P("det", None),
        P("det", None),
    )
    return jax.shard_map(
        on_device, mesh=mesh, in_specs=placed, out_specs=P("det", "bm"), check_vma=False
    )
```

```python
import functools
import math

import jax
import jax.numpy as jnp
from jax import lax
from jax.experimental import pallas as pl
from jax.experimental.pallas import tpu as pltpu
from jax.sharding import PartitionSpec as P

NPHI = 16384
NPSI = 32

TWO_PI = 2.0 * math.pi
LANES = 128
ROWS = 8
PUSH_BYTES = 1 << 18
F32 = jnp.float32
BF16 = jnp.bfloat16
MESH = pl.DeviceIdType.MESH


def cos_on_grid(step, grid):
    shift = (grid // 4).bit_length() - 1
    turn = (step + grid // 8) >> shift
    x = (step - (turn << shift)).astype(F32) * (TWO_PI / grid)
    x2 = x * x
    c = 1.0 + x2 * (-0.5 + x2 * (1 / 24 + x2 * (-1 / 720 + x2 * (1 / 40320))))
    s = x * (1.0 + x2 * (-1 / 6 + x2 * (1 / 120 + x2 * (-1 / 5040 + x2 * (1 / 362880)))))
    odd = (turn & 1) == 1
    value = jnp.where(odd, -s, c)
    return jnp.where((turn & 2) == 2, -value, value)


def partner(me, flip, n):
    out, bit = 0, 1
    while bit < n:
        digit = (me // bit) % 2
        out = out + bit * ((1 - digit) if flip & bit else digit)
        bit *= 2
    return out


def rows_of(values, groups, width):
    return jnp.concatenate([values[j * ROWS : (j + 1) * ROWS] for j in range(groups)], axis=1)


def pushed(role, n_bm, source, target):
    even, inner = role
    top = even & (source == n_bm - 1)
    return (source > target) & ((target == 0) | top | (inner & (source - target >= 2)))


def kernel(
    n_det, n_bm, modes, pushes,
    sky_hbm, beam_hbm, wig_hbm, theta_hbm, phi_hbm, psi_hbm, out_ref,
    sky_all, slab, index, sky_wide, wide, feat, phase, cube_all, early, left,
    sky_sem, col_send, col_recv, ok, hello,
):
    det = lax.axis_index("det")
    bm = lax.axis_index("bm")
    even = det % 2 == 0
    pair = det // 2
    buddy = det + 1 - 2 * (det % 2)
    n_pairs = n_det // 2
    role = even, even | (pair != n_pairs - 1)

    cycles, units, _, band = wig_hbm.shape
    beam_units = beam_hbm.shape[0]
    planes = beam_units * ROWS // 6
    owned = sky_all.shape[3]
    chunks = n_pairs if pushes else 1
    part_units = units // chunks
    chunk_units = cycles * part_units
    wig_units = cycles * units
    pairs = cycles * planes
    depth = 2 * pairs
    per_tile = LANES // (2 * depth)
    tile_modes = per_tile * ROWS
    tiles = modes // tile_modes
    dets, samples = index.shape[1:]
    width = samples // n_bm
    groups = dets // ROWS

    load = pltpu.make_async_copy(sky_hbm, sky_all.at[det], sky_sem.at[0])

    def place_of(k):
        return partner(pair, k, n_pairs) if pushes else 0

    lead_sem = col_send.at[(bm + n_bm - 1) % n_bm]

    def fetch(k):
        pltpu.make_async_copy(
            wig_hbm.at[:, pl.ds(place_of(k) * part_units, part_units)],
            slab.at[bm, pl.ds(k * chunk_units, chunk_units)].reshape(cycles, part_units, ROWS, band),
            lead_sem if k == 1 else col_send.at[bm],
        ).start()

    def fetch_all():
        for k in range(2, chunks):
            fetch(k)
        pltpu.make_async_copy(
            beam_hbm, slab.at[bm, pl.ds(wig_units, beam_units)], col_send.at[bm]
        ).start()
        fetch(0)

    last = pair == n_pairs - 1

    ahead = even & jnp.logical_not(last)

    @pl.when(ahead)
    def _():
        if pushes:
            fetch(1)
        load.start()
        fetch_all()

    @pl.when(jnp.logical_not(ahead))
    def _():
        load.start()

    @pl.when(jnp.logical_not(even | last))
    def _():
        if pushes:
            fetch(1)
        fetch_all()

    barrier = pltpu.get_barrier_semaphore()

    def greet(semaphore, to_det, to_bm):
        pl.semaphore_signal(semaphore, inc=1, device_id=(to_det, to_bm), device_id_type=MESH)

    greet(barrier, buddy, bm)
    for z in range(1, n_bm):
        @pl.when(bm < z)
        def _():
            greet(barrier, 2 * pair + 1, z)
    for k in range(1, n_pairs):
        greet(barrier, 2 * ((pair + k) % n_pairs), bm)

    @pl.when(last)
    def _():
        if pushes:
            fetch(1)
        fetch_all()

    slab_units = wig_units + beam_units
    sent_units = slab_units - chunk_units

    def push_to(z, first=chunk_units, stop=slab_units):
        part = slab.at[bm, pl.ds(first, stop - first)]
        return pltpu.make_async_remote_copy(
            src_ref=part, dst_ref=part,
            send_sem=col_send.at[z], recv_sem=col_recv.at[bm],
            device_id=(det, z), device_id_type=MESH,
        )

    def early_to(z):
        return pltpu.make_async_remote_copy(
            src_ref=early.at[bm], dst_ref=early.at[bm],
            send_sem=col_send.at[z], recv_sem=col_recv.at[bm],
            device_id=(det, z), device_id_type=MESH,
        )

    def cube_to(z):
        return pltpu.make_async_remote_copy(
            src_ref=cube_all.at[bm], dst_ref=cube_all.at[bm],
            send_sem=col_send.at[z], recv_sem=col_recv.at[bm],
            device_id=(det, z), device_id_type=MESH,
        )

    def landing(buffer, z):
        return pltpu.make_async_remote_copy(
            src_ref=buffer, dst_ref=buffer,
            send_sem=col_send.at[z], recv_sem=col_recv.at[z],
            device_id=(det, z), device_id_type=MESH,
        )

    early_units = ROWS * LANES * 4 // (ROWS * band * 2)
    moved = slab.at[bm, pl.ds(0, sent_units + early_units)]

    @pl.when(jnp.logical_not(even))
    def _():
        pl.semaphore_wait(barrier, 1 + 2 * bm)
        greet(ok, buddy, bm)

    @pl.when(even)
    def _():
        pl.semaphore_wait(ok, 1)

    if pushes:
        yields = jnp.logical_not(even) & (pair == 0) & (bm == n_bm - 1)
        at_once = jnp.logical_not(yields) & pushed(role, n_bm, bm, 0)

    def share_lead():
        part = slab.at[bm, pl.ds(chunk_units, chunk_units)]
        pltpu.make_async_copy(part, part, lead_sem).wait()

        @pl.when(at_once)
        def _():
            push_to(0, chunk_units, 2 * chunk_units).start()

    if pushes:
        @pl.when(ahead)
        def _():
            share_lead()

    load.wait()
    to_buddy = pltpu.make_async_remote_copy(
        src_ref=sky_all.at[det], dst_ref=sky_all.at[det],
        send_sem=sky_sem.at[0], recv_sem=sky_sem.at[2],
        device_id=(buddy, bm), device_id_type=MESH,
    )
    to_buddy.start()
    pltpu.make_async_copy(theta_hbm, index.at[0], col_recv.at[bm]).start()
    pltpu.make_async_copy(phi_hbm, index.at[1], col_recv.at[bm]).start()
    pltpu.make_async_copy(psi_hbm, index.at[2], col_recv.at[bm]).start()

    def share_sky():
        @pl.when(even)
        def _():
            pl.semaphore_wait(barrier, n_det - 1)
            greet(ok, buddy, bm)

        @pl.when(jnp.logical_not(even))
        def _():
            pl.semaphore_wait(ok, 1)

        for flip in range(n_det - 1, 1, -1):
            pltpu.make_async_remote_copy(
                src_ref=sky_all.at[det], dst_ref=sky_all.at[det],
                send_sem=sky_sem.at[0], recv_sem=sky_sem.at[1],
                device_id=(partner(det, flip, n_det), bm), device_id_type=MESH,
            ).start()

    lane = lax.broadcasted_iota(jnp.int32, (ROWS, LANES), 1)
    blocks = 2 * per_tile
    imag_row = (lane // (depth * per_tile)) % 2
    sin_column = (lane // pairs) % 2
    part = (imag_row + sin_column) % 2
    code = ((lane // depth) % per_tile * 2 + part) * pairs + lane % pairs
    sign = jnp.where((imag_row == 0) & (sin_column == 1), -1.0, 1.0)
    sign_column = jnp.where(sin_column == 1, -1.0, 1.0)

    def widen(z, first):
        for k in range(first, chunks):
            rows = pl.ds(pl.multiple_of(place_of(k) * part_units * ROWS, ROWS), part_units * ROWS)
            for g in range(cycles):
                block = slab[z, pl.ds(k * chunk_units + g * part_units, part_units)]
                wide[g, rows] = block.astype(F32).reshape(part_units * ROWS, band)

    def totals(z, sky, at):
        beam = slab[z, pl.ds(wig_units, beam_units)].astype(F32).reshape(beam_units * ROWS, band)
        for p in range(planes):
            re = im = 0.0
            for c in range(3):
                b0 = beam[c * planes + p : c * planes + p + 1]
                b1 = beam[(3 + c) * planes + p : (3 + c) * planes + p + 1]
                re = re + (sky[0][c] * b0 - sky[1][c] * b1)
                im = im + (sky[0][c] * b1 + sky[1][c] * b0)
            re = re.astype(BF16).astype(F32)
            im = im.astype(BF16).astype(F32)
            for g in range(cycles):
                w = wide[g, pl.ds(at * planes + p, ROWS, stride=planes)]
                for k, spectra in enumerate((re, im)):
                    yield k, g * planes + p, jnp.sum(w * spectra, axis=1, keepdims=True)

    shared = 2 * owned
    own_group = pair * shared // ROWS

    def send_early():
        to_buddy.wait_recv()
        near = [
            [
                sky_all[pl.ds(2 * pair, 2), r, c].astype(F32).reshape(shared, band)
                for c in range(3)
            ]
            for r in range(2)
        ]
        sky = [[jnp.concatenate([x] * (ROWS // shared), axis=0) for x in y] for y in near]
        packed = jnp.zeros((ROWS, LANES), F32)
        for k, i, total in totals(bm, sky, pl.multiple_of(own_group * ROWS, ROWS)):
            packed = jnp.where(part * pairs + lane % pairs == k * pairs + i, total, packed)
        early[bm] = packed * sign
        early_to(0).start()

    def share_slab():
        if pushes:
            @pl.when(jnp.logical_not(ahead))
            def _():
                share_lead()

        rest = slab.at[bm, pl.ds(0, slab_units - chunk_units if pushes else slab_units)]
        pltpu.make_async_copy(rest, rest, col_send.at[bm]).wait()
        if pushes:
            @pl.when(at_once)
            def _():
                push_to(0, 2 * chunk_units).start()
        for z in range(n_bm - 1):
            @pl.when(bm > z)
            def _():
                greet(hello, det, z)
        widen(bm, 0)
        if pushes:
            @pl.when(pushed(role, n_bm, bm, 0))
            def _():
                send_early()

            @pl.when(yields & pushed(role, n_bm, bm, 0))
            def _():
                push_to(0).start()

    @pl.when(last)
    def _():
        share_sky()

    share_slab()

    @pl.when(jnp.logical_not(last))
    def _():
        share_sky()

    def share_inner(now):
        for z in range(1, n_bm - 1):
            @pl.when(now & pushed(role, n_bm, bm, z))
            def _():
                push_to(z).start()
                early_to(z).start()

    if pushes:
        share_inner((pair == 0) | jnp.logical_not(even))

    others = sky_all.at[pl.ds(0, n_det - 2)]
    skies = pltpu.make_async_remote_copy(
        src_ref=others, dst_ref=others,
        send_sem=sky_sem.at[0], recv_sem=sky_sem.at[1],
        device_id=(buddy, bm), device_id_type=MESH,
    )
    pltpu.make_async_copy(index, index, col_recv.at[bm]).wait()

    def mine(values):
        own = values[:, :width]
        for i in range(1, n_bm):
            own = jnp.where(bm == i, values[:, i * width : (i + 1) * width], own)
        return rows_of(own, groups, width)

    theta, phi, psi = mine(index[0]), mine(index[1]), mine(index[2])
    span = groups * width
    k_rows = n_bm * depth
    row = lax.broadcasted_iota(jnp.int32, (k_rows, span), 0)
    plane = row // depth * planes + row % planes
    cycle = (row // planes) % cycles
    quarter = ((row // pairs) % 2) * (3 * NPSI // 4)
    m_rows = 2 * modes
    mrow = lax.broadcasted_iota(jnp.int32, (m_rows, span), 0)
    mode = (mrow // (2 * tile_modes)) * tile_modes + mrow % tile_modes
    mquarter = ((mrow // tile_modes) % 2) * (NPHI // 4)
    for j in range(ROWS):
        at = pl.ds(j * span, span)
        step = (plane * psi[j : j + 1] + quarter) & (NPSI - 1)
        value = jnp.where(cycle == theta[j : j + 1], cos_on_grid(step, NPSI), 0.0)
        feat[:, at] = value.astype(BF16)
        step = (mode * phi[j : j + 1] + mquarter) & (NPHI - 1)
        phase[:, at] = cos_on_grid(step, NPHI)

    if pushes:
        share_inner((pair != 0) & even)

        @pl.when(jnp.logical_not(pushed(role, n_bm, bm, 0)))
        def _():
            to_buddy.wait_recv()
    else:
        to_buddy.wait_recv()
    skies.wait_recv()

    slots = tile_modes // owned
    for t in range(tiles):
        for r in range(2):
            for c in range(3):
                sky_wide[r, c, pl.ds(t * tile_modes, tile_modes)] = (
                    sky_all[t * slots : (t + 1) * slots, r, c].astype(F32).reshape(tile_modes, band)
                )

    def tile_totals(z, t, h):
        at = t * tile_modes + h * ROWS
        sky = [[sky_wide[r, c, pl.ds(at, ROWS)] for c in range(3)] for r in range(2)]
        return totals(z, sky, at)

    def profile(z):
        for t in range(tiles):
            packed = jnp.zeros((ROWS, LANES), F32)
            for h in range(per_tile):
                for k, i, total in tile_totals(z, t, h):
                    packed = jnp.where(code == (h * 2 + k) * pairs + i, total, packed)
            cube_all[z, t] = packed * sign

    def profile_here(z):
        inner = lane - z * depth
        inside = lane // depth == z
        for t in range(tiles):
            for h in range(per_tile):
                real = imag = jnp.zeros((ROWS, LANES), F32)
                for k, i, total in tile_totals(z, t, h):
                    cos_place, sin_place = inner == i, inner == pairs + i
                    real = jnp.where(sin_place if k else cos_place, total, real)
                    imag = jnp.where(cos_place if k else sin_place, total, imag)
                left[t, h] = jnp.where(inside, real * sign_column, left[t, h])
                left[t, per_tile + h] = jnp.where(inside, imag, left[t, per_tile + h])
        row = lax.broadcasted_iota(jnp.int32, (ROWS, LANES), 0)
        known = inside & (row // shared == pair % (ROWS // shared))
        for q in range(blocks):
            ready = pltpu.roll(early[z], (z - q) % n_bm * depth, 1)
            left[0, q] = jnp.where(known & (own_group == q % per_tile), ready, left[0, q])

    def place(z):
        inside = lane // depth == z
        for t in range(tiles):
            for q in range(blocks):
                moved = pltpu.roll(cube_all[z, t], (z - q) % n_bm * depth, 1)
                left[t, q] = jnp.where(inside, moved, left[t, q])

    profile(bm)

    @pl.when(bm < n_bm - 1)
    def _():
        pl.semaphore_wait(hello, n_bm - 1 - bm)

    def by_cube(source, target):
        apart = source != target
        return apart & jnp.logical_not(pushed(role, n_bm, source, target)) if pushes else apart

    for z in range(n_bm - 1, -1, -1):
        @pl.when(by_cube(bm, z))
        def _():
            cube_to(z).start()

    left[...] = jnp.zeros_like(left)
    for z in range(n_bm):
        @pl.when(bm == z)
        def _():
            place(z)

    def take(z):
        landing(moved, z).wait_recv()
        widen(z, 1)
        profile_here(z)

    def finish():
        wave = left[...].reshape(m_rows, k_rows)
        high = wave.astype(BF16)
        low = (wave - high.astype(F32)).astype(BF16)
        both = jnp.concatenate([high, low], axis=0)
        y = jnp.dot(both, feat[...], preferred_element_type=F32)
        terms = (y[:m_rows] + y[m_rows:]) * phase[...]
        total = jnp.sum(terms, axis=0, keepdims=True)
        for j in range(ROWS):
            for i in range(groups):
                at = j * span + i * width
                out_ref[pl.ds(i * ROWS + j, 1), :] = total[:, at : at + width]

    def finish_mixed():
        if pushes:
            for z in range(1, n_bm):
                @pl.when(pushed(role, n_bm, z, bm))
                def _():
                    take(z)
        for z in range(n_bm):
            @pl.when(by_cube(z, bm))
            def _():
                landing(cube_all.at[z], z).wait_recv()
                place(z)
        finish()

    if pushes:
        @pl.when(bm == 0)
        def _():
            for z in range(1, n_bm):
                take(z)
            finish()

        @pl.when(bm > 0)
        def _():
            finish_mixed()
    else:
        finish_mixed()

    every = sky_all.at[pl.ds(0, n_det - 1)]
    outbound = pltpu.make_async_remote_copy(
        src_ref=every, dst_ref=every,
        send_sem=sky_sem.at[0], recv_sem=sky_sem.at[1],
        device_id=(buddy, bm), device_id_type=MESH,
    )
    outbound.wait_send()
    for z in range(n_bm):
        @pl.when(by_cube(bm, z))
        def _():
            cube_to(z).wait_send()
        if pushes and z < n_bm - 1:
            @pl.when(pushed(role, n_bm, bm, z))
            def _():
                landing(moved, z).wait_send()


def on_device(sky_alm, beam_blm, wigner, theta_index, phi_index, psi_index):
    n_det, n_bm = lax.axis_size("det"), lax.axis_size("bm")
    cycles, modes, planes, band = wigner.shape
    dets, samples = theta_index.shape
    width = samples // n_bm
    span = dets // ROWS * width
    depth = 2 * cycles * planes
    tiles = modes * 2 * depth // (ROWS * LANES)
    beam_rows = 6 * planes
    units = modes * planes // ROWS
    wig_units = cycles * units
    beam_units = beam_rows // ROWS
    pushes = tiles == 1 and 2 * wig_units * ROWS * band <= PUSH_BYTES
    any_space = pl.BlockSpec(memory_space=pl.ANY)
    return pl.pallas_call(
        functools.partial(kernel, n_det, n_bm, modes, pushes),
        out_shape=pltpu.VMEM((dets, width), F32),
        in_specs=[any_space] * 6,
        out_specs=pl.BlockSpec(memory_space=pltpu.VMEM),
        scratch_shapes=[
            pltpu.VMEM((n_det, *sky_alm.shape), BF16),
            pltpu.VMEM((n_bm, wig_units + beam_units, ROWS, band), BF16),
            pltpu.VMEM((3, dets, samples), jnp.int32),
            pltpu.VMEM((2, 3, modes, band), F32),
            pltpu.VMEM((cycles, modes * planes, band), F32),
            pltpu.VMEM((n_bm * depth, ROWS * span), BF16),
            pltpu.VMEM((2 * modes, ROWS * span), F32),
            pltpu.VMEM((n_bm, tiles, ROWS, LANES), F32),
            pltpu.VMEM((n_bm, ROWS, LANES), F32),
            pltpu.VMEM((tiles, LANES // depth, ROWS, LANES), F32),
            pltpu.SemaphoreType.DMA((3,)),
            pltpu.SemaphoreType.DMA((n_bm,)),
            pltpu.SemaphoreType.DMA((n_bm,)),
            pltpu.SemaphoreType.REGULAR,
            pltpu.SemaphoreType.REGULAR,
        ],
        compiler_params=pltpu.CompilerParams(collective_id=0, has_side_effects=True),
    )(
        sky_alm,
        beam_blm.reshape(beam_units, ROWS, band),
        wigner.reshape(cycles, units, ROWS, band),
        theta_index,
        phi_index,
        psi_index,
    )


def solution(mesh):
    placed = (
        P(None, None, "det", None),
        P(None, None, "bm", None),
        P("det", None, "bm", None),
        P("det", None),
        P("det", None),
        P("det", None),
    )
    return jax.shard_map(
        on_device, mesh=mesh, in_specs=placed, out_specs=P("det", "bm"), check_vma=False
    )
```
